32 devices in a mesh: dp: 4 (over y, z), sp: 8 (over x, core).
Axes of the slice: x: 4, y: 2, z: 2, core: 2. Of those that a mesh axis runs over, the one named last changes fastest.
The devices are a block of a 4x4x8 slice.
Arguments:
- x_in: bfloat16 [8192, 2560], P(('dp', 'sp')), parts along dimension 0
- seg_id: int32 [8192], P(('dp', 'sp')), parts along dimension 0
- pos_id: int32 [8192], P(('dp', 'sp')), parts along dimension 0
- w_dq: bfloat16 [2560, 768], replicated
- g_q: bfloat16 [768], replicated
- w_uq: bfloat16 [768, 24576], replicated
- w_dkv: bfloat16 [2560, 576], replicated
- g_kv: bfloat16 [512], replicated
- w_ukv: bfloat16 [512, 32768], replicated
- w_o: bfloat16 [16384, 2560], replicated
- g_ffn: bfloat16 [2560], replicated
- w_gate: bfloat16 [2560, 6144], P(None, 'sp')
- w_up: bfloat16 [2560, 6144], P(None, 'sp')
- w_down: bfloat16 [6144, 2560], P('sp')
Outputs:
- output: bfloat16 [8192, 2560], P(('dp', 'sp')), parts along dimension 0
There are 4 independent parts. The reference program is written for one: setup_inputs(seed, part) draws one part's arguments, and reference() takes and returns one part's arrays. A program takes and returns all parts, laid end to end along the dimension named above; an argument that names none is the same for every part.
All inputs are finite; a program needn't handle non-finite values.
Results may differ from the reference program's by a relative error of at most 0.0150041.
Values are sent between devices in bfloat16 or wider.
A program may use at most 768 MiB of HBM per device.

```python
import jax
import jax.numpy as jnp
from jax import lax

D = 2560
HEADS = 128
Q_LAT = 768
FF = 6144
TOKENS = 2048
KV_LATENT = 512
ROPE_DIM = 64
NOPE_DIM = 128
VALUE_DIM = 128
MAX_CUTS = 3
QK_DIM = NOPE_DIM + ROPE_DIM
KV_DIM = NOPE_DIM + VALUE_DIM


def rms_norm(vec_in, gain_vec):
    mean_sq = jnp.mean(vec_in * vec_in, axis=-1, keepdims=True)
    return vec_in * lax.rsqrt(mean_sq + 1e-6) * gain_vec.astype(jnp.float32)


def apply_rope(vec_in, positions):
    half_dim = ROPE_DIM // 2
    inv_freq = 10000.0 ** (-jnp.arange(half_dim, dtype=jnp.float32) / half_dim)
    angles = positions.astype(jnp.float32)[..., None] * inv_freq
    cosine = jnp.cos(angles)
    sine_v = jnp.sin(angles)
    lo_half = vec_in[..., :half_dim]
    hi_half = vec_in[..., half_dim:]
    return jnp.concatenate([lo_half * cosine - hi_half * sine_v, hi_half * cosine + lo_half * sine_v], axis=-1)


def draw_prompts(root_key):
    cut_key, count_key = jax.random.split(root_key)
    cut_at = jax.random.randint(cut_key, (MAX_CUTS,), 1, TOKENS)
    n_cuts = jax.random.randint(count_key, (), 1, MAX_CUTS + 1)
    cut_used = (jnp.arange(MAX_CUTS) < n_cuts).astype(jnp.int32)
    cut_marks = jnp.zeros((TOKENS,), jnp.int32).at[cut_at].max(cut_used)
    seg_id = jnp.cumsum(cut_marks).astype(jnp.int32)
    tok_index = jnp.arange(TOKENS, dtype=jnp.int32)
    starts = lax.cummax(jnp.where(cut_marks > 0, tok_index, 0), axis=0)
    return seg_id, (tok_index - starts).astype(jnp.int32)


def normal_weight(w_key, arr_shape, fan_in):
    return (jax.random.normal(w_key, arr_shape, jnp.float32) * fan_in ** -0.5).astype(jnp.bfloat16)


def gain_draw(w_key, arr_shape):
    return jax.random.uniform(w_key, arr_shape, jnp.float32, 0.5, 1.5).astype(jnp.bfloat16)


def setup_inputs(seed: int = 0, part: int = 0) -> dict:
    root_key = jax.random.key(seed)
    shared_key, part_root = jax.random.split(root_key)
    part_key = jax.random.fold_in(part_root, part)
    x_key, prompt_key = jax.random.split(part_key)
    sub_keys = jax.random.split(shared_key, 11)
    seg_id, pos_id = draw_prompts(prompt_key)
    return {
        'x_in': jax.random.normal(x_key, (TOKENS, D), jnp.float32).astype(jnp.bfloat16),
        'seg_id': seg_id,
        'pos_id': pos_id,
        'w_dq': normal_weight(sub_keys[0], (D, Q_LAT), D),
        'g_q': gain_draw(sub_keys[1], (Q_LAT,)),
        'w_uq': normal_weight(sub_keys[2], (Q_LAT, HEADS * QK_DIM), Q_LAT),
        'w_dkv': normal_weight(sub_keys[3], (D, KV_LATENT + ROPE_DIM), D),
        'g_kv': gain_draw(sub_keys[4], (KV_LATENT,)),
        'w_ukv': normal_weight(sub_keys[5], (KV_LATENT, HEADS * KV_DIM), KV_LATENT),
        'w_o': normal_weight(sub_keys[6], (HEADS * VALUE_DIM, D), HEADS * VALUE_DIM),
        'g_ffn': gain_draw(sub_keys[7], (D,)),
        'w_gate': normal_weight(sub_keys[8], (D, FF), D),
        'w_up': normal_weight(sub_keys[9], (D, FF), D),
        'w_down': normal_weight(sub_keys[10], (FF, D), FF),
    }


def reference(x_in, seg_id, pos_id, w_dq, g_q, w_uq, w_dkv, g_kv, w_ukv, w_o, g_ffn, w_gate, w_up, w_down):
    q_lin = jnp.dot(x_in, w_dq, preferred_element_type=jnp.float32)
    c_q = rms_norm(q_lin, g_q).astype(jnp.bfloat16)
    kv_lin = jnp.dot(x_in, w_dkv, preferred_element_type=jnp.float32)
    c_kv = rms_norm(kv_lin[:, :KV_LATENT], g_kv).astype(jnp.bfloat16)
    k_rope = apply_rope(kv_lin[:, KV_LATENT:], pos_id).astype(jnp.bfloat16)
    allowed = (seg_id[:, None] == seg_id[None, :]) & (pos_id[None, :] <= pos_id[:, None])
    score_scale = QK_DIM ** -0.5
    w_uq_heads = jnp.transpose(w_uq.reshape(Q_LAT, HEADS, QK_DIM), (1, 0, 2))
    w_ukv_heads = jnp.transpose(w_ukv.reshape(KV_LATENT, HEADS, KV_DIM), (1, 0, 2))

    def one_head(weights):
        wq_head, wkv_head = weights
        q_head = jnp.dot(c_q, wq_head, preferred_element_type=jnp.float32)
        q_nope = q_head[:, :NOPE_DIM].astype(jnp.bfloat16)
        q_rope = apply_rope(q_head[:, NOPE_DIM:], pos_id).astype(jnp.bfloat16)
        kv_head = jnp.dot(c_kv, wkv_head, preferred_element_type=jnp.float32).astype(jnp.bfloat16)
        k_nope = kv_head[:, :NOPE_DIM]
        v_head = kv_head[:, NOPE_DIM:]
        scores = jnp.dot(q_nope, k_nope.T, preferred_element_type=jnp.float32) + jnp.dot(q_rope, k_rope.T, preferred_element_type=jnp.float32)
        scores = jnp.where(allowed, scores * score_scale, -jnp.inf)
        row_peak = jnp.max(scores, axis=1, keepdims=True)
        prob_w = jnp.exp(scores - row_peak)
        row_total = jnp.sum(prob_w, axis=1, keepdims=True)
        head_out = jnp.dot(prob_w.astype(jnp.bfloat16), v_head, preferred_element_type=jnp.float32) / row_total
        return head_out.astype(jnp.bfloat16)

    o_heads = lax.map(one_head, (w_uq_heads, w_ukv_heads))
    o_all = jnp.transpose(o_heads, (1, 0, 2)).reshape(TOKENS, HEADS * VALUE_DIM)
    y_att = jnp.dot(o_all, w_o, preferred_element_type=jnp.float32).astype(jnp.bfloat16)
    h_ffn = rms_norm(y_att.astype(jnp.float32), g_ffn).astype(jnp.bfloat16)
    gate_lin = jnp.dot(h_ffn, w_gate, preferred_element_type=jnp.float32)
    up_lin = jnp.dot(h_ffn, w_up, preferred_element_type=jnp.float32)
    act_val = (jax.nn.silu(gate_lin) * up_lin).astype(jnp.bfloat16)
    ffn_out = jnp.dot(act_val, w_down, preferred_element_type=jnp.float32)
    return (y_att.astype(jnp.float32) + ffn_out).astype(jnp.bfloat16)
```

```python
import functools
import jax
import jax.numpy as jnp
from jax import lax
from jax.experimental import pallas as pl
from jax.experimental.pallas import tpu as pltpu
from jax.sharding import PartitionSpec as P

NOPE_DIM = 128
ROPE_DIM = 64
VALUE_DIM = 128
KV_LATENT = 512
QK_DIM = NOPE_DIM + ROPE_DIM
KV_DIM = NOPE_DIM + VALUE_DIM
SCORE_SCALE = QK_DIM ** -0.5
LOG2E = 1.4426950408889634
NEG = -2.0e38
F32 = jnp.float32
BF16 = jnp.bfloat16


def rms_norm(vec_in, gain_vec):
    mean_sq = jnp.mean(vec_in * vec_in, axis=-1, keepdims=True)
    return vec_in * lax.rsqrt(mean_sq + 1e-6) * gain_vec.astype(F32)


def rope_tables(positions):
    half_dim = ROPE_DIM // 2
    inv_freq = 10000.0 ** (-jnp.arange(half_dim, dtype=F32) / half_dim)
    angles = positions.astype(F32)[..., None] * inv_freq
    return jnp.cos(angles), jnp.sin(angles)


def attn_body(core_ref, lo_ref, mid_ref, blk_ref, ckv_ref, kr_ref, cqa_ref, cqb_ref, cos_ref, sin_ref, start_ref,
              wuq_ref, wukv_ref, o_ref, kcat, vt, qcat, acc):
    i = pl.program_id(0)
    tok = ckv_ref.shape[0]
    qb = cqa_ref.shape[0]
    kb = qb

    @pl.when(i == 0)
    def _():
        kr = kr_ref[...]
        pad = jnp.concatenate([kr, jnp.zeros_like(kr)], axis=1)
        for h in range(2):
            kcat[h, :, NOPE_DIM:] = pad

    for r in range(tok // 512):
        rows = pl.ds(r * 512, 512)
        e = jnp.dot(ckv_ref[rows, :], wukv_ref[...], preferred_element_type=F32).astype(BF16)
        for h in range(2):
            kcat[h, rows, :NOPE_DIM] = e[:, KV_DIM * h:KV_DIM * h + NOPE_DIM]
            vt[h, :, rows] = e[:, KV_DIM * h + NOPE_DIM:KV_DIM * (h + 1)].T

    for b, cq in enumerate((cqa_ref, cqb_ref)):
        rows = pl.ds(b * qb, qb)
        q = jnp.dot(cq[...], wuq_ref[...], preferred_element_type=F32)
        q_r = jnp.concatenate([q[:, NOPE_DIM:QK_DIM], q[:, QK_DIM + NOPE_DIM:]], axis=1)
        lane = lax.broadcasted_iota(jnp.int32, q_r.shape, 1)
        lo_half = (lane % ROPE_DIM) < (ROPE_DIM // 2)
        swapped = jnp.where(lo_half, pltpu.roll(q_r, 2 * ROPE_DIM - ROPE_DIM // 2, 1), pltpu.roll(q_r, ROPE_DIM // 2, 1))
        q_r = (q_r * cos_ref[rows, :] + swapped * sin_ref[rows, :]).astype(BF16)
        zero = jnp.zeros((qb, ROPE_DIM), BF16)
        for h in range(2):
            qcat[h, rows, :NOPE_DIM] = q[:, QK_DIM * h:QK_DIM * h + NOPE_DIM].astype(BF16)
            qcat[h, rows, NOPE_DIM:] = jnp.concatenate([q_r[:, ROPE_DIM * h:ROPE_DIM * (h + 1)], zero], axis=1)

    for b in range(2):
        qrows = pl.ds(b * qb, qb)
        t0 = blk_ref[b] * qb

        def step(j, carry, masked):
            k0 = pl.multiple_of(j * kb, kb)
            krows = pl.ds(k0, kb)
            new = []
            for h in range(2):
                m, l = carry[2 * h], carry[2 * h + 1]
                s = lax.dot_general(kcat[h, krows, :], qcat[h, qrows, :], (((1,), (1,)), ((), ())),
                                    preferred_element_type=F32)
                s = s * (SCORE_SCALE * LOG2E)
                if masked:
                    r = k0 + lax.broadcasted_iota(jnp.int32, s.shape, 0)
                    t = t0 + lax.broadcasted_iota(jnp.int32, s.shape, 1)
                    s = jnp.where((r <= t) & (r >= start_ref[:, qrows]), s, NEG)
                m_new = jnp.maximum(m, jnp.max(s, axis=0, keepdims=True))
                alpha = jnp.exp2(m - m_new)
                p = jnp.exp2(s - m_new)
                l = alpha * l + jnp.sum(p, axis=0, keepdims=True)
                acc[h] = acc[h] * alpha + jnp.dot(vt[h, :, krows], p.astype(BF16), preferred_element_type=F32)
                new += [m_new, l]
            return tuple(new)

        acc[...] = jnp.zeros_like(acc)
        init = (jnp.full((1, qb), NEG, F32), jnp.zeros((1, qb), F32)) * 2
        carry = lax.fori_loop(lo_ref[b], mid_ref[b], functools.partial(step, masked=True), init)
        carry = lax.fori_loop(mid_ref[b], blk_ref[b], functools.partial(step, masked=False), carry)
        carry = step(blk_ref[b], carry, True)
        for h in range(2):
            o = (acc[h] * (1.0 / carry[2 * h + 1])).astype(BF16)
            o_ref[qrows, VALUE_DIM * h:VALUE_DIM * (h + 1)] = o.T


def attention(core, lo, mid, blk, ckv, kr, cqa, cqb, cos, sin, start, w_uq, w_ukv):
    tok = ckv.shape[0]
    qb, q_lat = cqa.shape
    heads = w_uq.shape[1] // QK_DIM
    pairs = heads // 4
    full = lambda shape: pl.BlockSpec(shape, lambda i, *_: (0, 0))
    return pl.pallas_call(
        attn_body,
        grid_spec=pltpu.PrefetchScalarGridSpec(
            num_scalar_prefetch=4,
            grid=(pairs,),
            in_specs=[
                full(ckv.shape), full(kr.shape), full(cqa.shape), full(cqb.shape), full(cos.shape), full(sin.shape),
                full(start.shape),
                pl.BlockSpec((q_lat, 2 * QK_DIM), lambda i, core, *_: (0, core[0] * pairs + i)),
                pl.BlockSpec((KV_LATENT, 2 * KV_DIM), lambda i, core, *_: (0, core[0] * pairs + i)),
            ],
            out_specs=pl.BlockSpec((2 * qb, 2 * VALUE_DIM), lambda i, *_: (0, i)),
            scratch_shapes=[
                pltpu.VMEM((2, tok, 2 * NOPE_DIM), BF16),
                pltpu.VMEM((2, VALUE_DIM, tok), BF16),
                pltpu.VMEM((2, 2 * qb, 2 * NOPE_DIM), BF16),
                pltpu.VMEM((2, VALUE_DIM, qb), F32),
            ]),
        out_shape=jax.ShapeDtypeStruct((2 * qb, heads // 2 * VALUE_DIM), BF16),
        compiler_params=pltpu.CompilerParams(dimension_semantics=("arbitrary",), vmem_limit_bytes=60 * 2 ** 20),
        cost_estimate=pl.CostEstimate(flops=80 * 10 ** 9, bytes_accessed=45 * 10 ** 6, transcendentals=40 * 10 ** 6),
    )(core, lo, mid, blk, ckv, kr, cqa, cqb, cos, sin, start, w_uq, w_ukv)


def wo_body(core_ref, o_ref, w_ref, y_ref):
    @pl.when(pl.program_id(1) == 0)
    def _():
        y_ref[...] = jnp.zeros_like(y_ref)
    y_ref[...] += jnp.dot(o_ref[...], w_ref[...], preferred_element_type=F32)


def wo_matmul(core, o, w_o, tn=1280, tk=1024):
    rows, depth = o.shape
    cols = w_o.shape[1]
    nk = depth // tk
    return pl.pallas_call(
        wo_body,
        grid_spec=pltpu.PrefetchScalarGridSpec(
            num_scalar_prefetch=1,
            grid=(cols // tn, nk),
            in_specs=[pl.BlockSpec((rows, tk), lambda n, k, core: (0, k)),
                      pl.BlockSpec((tk, tn), lambda n, k, core: (core[0] * nk + k, n))],
            out_specs=pl.BlockSpec((rows, tn), lambda n, k, core: (0, n))),
        out_shape=jax.ShapeDtypeStruct((rows, cols), F32),
        compiler_params=pltpu.CompilerParams(dimension_semantics=("arbitrary", "arbitrary"),
                                             vmem_limit_bytes=60 * 2 ** 20),
        cost_estimate=pl.CostEstimate(flops=2 * rows * depth * cols, bytes_accessed=2 * depth * cols,
                                      transcendentals=0),
    )(core, o, w_o)


def solution(mesh):
    group_size = mesh.shape['sp']
    chips = group_size // 2
    tok_spec = P(('dp', 'sp'), None)
    row_spec = P(('dp', 'sp'))
    full_spec = P()
    col_spec = P(None, 'sp')
    pair_groups = [[2 * c, 2 * c + 1] for c in range(chips)]
    core_groups = [[2 * c + k for c in range(chips)] for k in range(2)]
    swap = [(d, d ^ 1) for d in range(group_size)]

    def device_fn(x_blk, seg_blk, pos_blk, w_dq, g_q, w_uq, w_dkv, g_kv, w_ukv, w_o, g_ffn, w_gate, w_up, w_down):
        me = lax.axis_index('sp')
        chip, core = me // 2, me % 2
        blk_len = x_blk.shape[0]
        core_arr = core.reshape(1).astype(jnp.int32)

        w_gate2 = lax.ppermute(w_gate, 'sp', swap)
        w_up2 = lax.ppermute(w_up, 'sp', swap)
        w_down2 = lax.ppermute(w_down, 'sp', swap)

        q_lin = jnp.dot(x_blk, w_dq, preferred_element_type=F32)
        c_q = rms_norm(q_lin, g_q).astype(BF16)
        kv_lin = jnp.dot(x_blk, w_dkv, preferred_element_type=F32)
        c_kv = rms_norm(kv_lin[:, :KV_LATENT], g_kv).astype(BF16)
        cosine, sine = rope_tables(pos_blk)
        lo_half, hi_half = kv_lin[:, KV_LATENT:KV_LATENT + ROPE_DIM // 2], kv_lin[:, KV_LATENT + ROPE_DIM // 2:]
        k_rope = jnp.concatenate([lo_half * cosine - hi_half * sine, hi_half * cosine + lo_half * sine],
                                 axis=-1).astype(BF16)
        gather = lambda a: lax.all_gather(a, 'sp', axis=0, tiled=True)
        cq_all, ckv_all, kr_all, pos_all = gather(c_q), gather(c_kv), gather(k_rope), gather(pos_blk)

        blk = jnp.stack([2 * chip, group_size - 1 - 2 * chip]).astype(jnp.int32)
        take = lambda a, b: lax.dynamic_slice_in_dim(a, blk[b] * blk_len, blk_len, axis=0)
        cqa, cqb = take(cq_all, 0), take(cq_all, 1)
        pos_q = jnp.concatenate([take(pos_all, 0), take(pos_all, 1)])
        rows_q = (blk[:, None] * blk_len + jnp.arange(blk_len, dtype=jnp.int32)[None, :]).reshape(-1)
        start = rows_q - pos_q
        cosine, sine = rope_tables(pos_q)
        cos4 = jnp.concatenate([cosine] * 4, axis=1)
        sin4 = jnp.concatenate([-sine, sine, -sine, sine], axis=1)
        lo = start.reshape(2, blk_len)[:, 0] // blk_len
        last = start.reshape(2, blk_len)[:, -1]
        mid = jnp.minimum((last + blk_len - 1) // blk_len, blk)
        mid = jnp.maximum(mid, lo)

        o = attention(core_arr, lo, mid, blk, ckv_all, kr_all, cqa, cqb, cos4, sin4, start[None, :], w_uq, w_ukv)
        y_part = wo_matmul(core_arr, o, w_o)
        y = lax.psum_scatter(y_part, 'sp', scatter_dimension=0, axis_index_groups=pair_groups, tiled=True).astype(BF16)
        y_all = lax.all_gather(y, 'sp', axis=0, axis_index_groups=core_groups, tiled=True)
        h_all = rms_norm(y_all.astype(F32), g_ffn).astype(BF16)

        def ffn(wg, wu, wd):
            gate_lin = jnp.dot(h_all, wg, preferred_element_type=F32)
            up_lin = jnp.dot(h_all, wu, preferred_element_type=F32)
            act_val = (jax.nn.silu(gate_lin) * up_lin).astype(BF16)
            return jnp.dot(act_val, wd, preferred_element_type=F32)

        part_sum = ffn(w_gate, w_up, w_down) + ffn(w_gate2, w_up2, w_down2)
        pick = jnp.where(core == 0, jnp.arange(chips), chips - 1 - jnp.arange(chips))
        part_sum = part_sum.reshape(chips, blk_len, -1)[pick].reshape(part_sum.shape)
        mine = jnp.where(core == 0, chip, chips - 1 - chip)
        y_own = lax.dynamic_slice_in_dim(y_all, mine * blk_len, blk_len, axis=0)
        ffn_out = lax.psum_scatter(part_sum, 'sp', scatter_dimension=0, axis_index_groups=core_groups, tiled=True)
        return (y_own.astype(F32) + ffn_out).astype(BF16)

    return jax.shard_map(device_fn, mesh=mesh, in_specs=(tok_spec, row_spec, row_spec, full_spec, full_spec, full_spec, full_spec, full_spec, full_spec, full_spec, full_spec, col_spec, col_spec, P('sp', None)), out_specs=tok_spec, check_vma=False)
```

```python
import functools
import jax
import jax.numpy as jnp
from jax import lax
from jax.experimental import pallas as pl
from jax.experimental.pallas import tpu as pltpu
from jax.sharding import PartitionSpec as P

NOPE_DIM = 128
ROPE_DIM = 64
VALUE_DIM = 128
KV_LATENT = 512
QK_DIM = NOPE_DIM + ROPE_DIM
KV_DIM = NOPE_DIM + VALUE_DIM
SCORE_SCALE = QK_DIM ** -0.5
LOG2E = 1.4426950408889634
NEG = -2.0e38
F32 = jnp.float32
BF16 = jnp.bfloat16


def rms_norm(vec_in, gain_vec):
    mean_sq = jnp.mean(vec_in * vec_in, axis=-1, keepdims=True)
    return vec_in * lax.rsqrt(mean_sq + 1e-6) * gain_vec.astype(F32)


def rope_tables(positions):
    half_dim = ROPE_DIM // 2
    inv_freq = 10000.0 ** (-jnp.arange(half_dim, dtype=F32) / half_dim)
    angles = positions.astype(F32)[..., None] * inv_freq
    return jnp.cos(angles), jnp.sin(angles)


def attn_body(core_ref, lo_ref, mid_ref, blk_ref, ckv_ref, kr_ref, cqa_ref, cqb_ref, cos_ref, sin_ref, start_ref,
              wuq_ref, wukv_ref, o_ref, kcat, vt, qcat, acc):
    i = pl.program_id(0)
    tok = ckv_ref.shape[0]
    qb = cqa_ref.shape[0]
    kb = qb

    @pl.when(i == 0)
    def _():
        kr = kr_ref[...]
        pad = jnp.concatenate([kr, jnp.zeros_like(kr)], axis=1)
        for h in range(2):
            kcat[h, :, NOPE_DIM:] = pad

    for r in range(tok // 512):
        rows = pl.ds(r * 512, 512)
        e = jnp.dot(ckv_ref[rows, :], wukv_ref[...], preferred_element_type=F32).astype(BF16)
        for h in range(2):
            kcat[h, rows, :NOPE_DIM] = e[:, KV_DIM * h:KV_DIM * h + NOPE_DIM]
            vt[h, :, rows] = e[:, KV_DIM * h + NOPE_DIM:KV_DIM * (h + 1)].T

    for b, cq in enumerate((cqa_ref, cqb_ref)):
        rows = pl.ds(b * qb, qb)
        q = jnp.dot(cq[...], wuq_ref[...], preferred_element_type=F32)
        q_r = jnp.concatenate([q[:, NOPE_DIM:QK_DIM], q[:, QK_DIM + NOPE_DIM:]], axis=1)
        lane = lax.broadcasted_iota(jnp.int32, q_r.shape, 1)
        lo_half = (lane % ROPE_DIM) < (ROPE_DIM // 2)
        swapped = jnp.where(lo_half, pltpu.roll(q_r, 2 * ROPE_DIM - ROPE_DIM // 2, 1), pltpu.roll(q_r, ROPE_DIM // 2, 1))
        q_r = (q_r * cos_ref[rows, :] + swapped * sin_ref[rows, :]).astype(BF16)
        zero = jnp.zeros((qb, ROPE_DIM), BF16)
        for h in range(2):
            qcat[h, rows, :NOPE_DIM] = q[:, QK_DIM * h:QK_DIM * h + NOPE_DIM].astype(BF16)
            qcat[h, rows, NOPE_DIM:] = jnp.concatenate([q_r[:, ROPE_DIM * h:ROPE_DIM * (h + 1)], zero], axis=1)

    for b in range(2):
        qrows = pl.ds(b * qb, qb)
        t0 = blk_ref[b] * qb

        def step(j, carry, masked):
            k0 = pl.multiple_of(j * kb, kb)
            krows = pl.ds(k0, kb)
            new = []
            for h in range(2):
                m, l = carry[2 * h], carry[2 * h + 1]
                s = lax.dot_general(kcat[h, krows, :], qcat[h, qrows, :], (((1,), (1,)), ((), ())),
                                    preferred_element_type=F32)
                s = s * (SCORE_SCALE * LOG2E)
                if masked:
                    r = k0 + lax.broadcasted_iota(jnp.int32, s.shape, 0)
                    t = t0 + lax.broadcasted_iota(jnp.int32, s.shape, 1)
                    s = jnp.where((r <= t) & (r >= start_ref[:, qrows]), s, NEG)
                m_new = jnp.maximum(m, jnp.max(s, axis=0, keepdims=True))
                alpha = jnp.exp2(m - m_new)
                p = jnp.exp2(s - m_new)
                l = alpha * l + jnp.sum(p, axis=0, keepdims=True)
                acc[h] = acc[h] * alpha + jnp.dot(vt[h, :, krows], p.astype(BF16), preferred_element_type=F32)
                new += [m_new, l]
            return tuple(new)

        acc[...] = jnp.zeros_like(acc)
        init = (jnp.full((1, qb), NEG, F32), jnp.zeros((1, qb), F32)) * 2
        carry = lax.fori_loop(lo_ref[b], mid_ref[b], functools.partial(step, masked=True), init)
        carry = lax.fori_loop(mid_ref[b], blk_ref[b], functools.partial(step, masked=False), carry)
        carry = step(blk_ref[b], carry, True)
        for h in range(2):
            o = (acc[h] * (1.0 / carry[2 * h + 1])).astype(BF16)
            o_ref[qrows, VALUE_DIM * h:VALUE_DIM * (h + 1)] = o.T


def attention(core, lo, mid, blk, ckv, kr, cqa, cqb, cos, sin, start, w_uq, w_ukv):
    tok = ckv.shape[0]
    qb, q_lat = cqa.shape
    heads = w_uq.shape[1] // QK_DIM
    pairs = heads // 4
    full = lambda shape: pl.BlockSpec(shape, lambda i, *_: (0, 0))
    return pl.pallas_call(
        attn_body,
        grid_spec=pltpu.PrefetchScalarGridSpec(
            num_scalar_prefetch=4,
            grid=(pairs,),
            in_specs=[
                full(ckv.shape), full(kr.shape), full(cqa.shape), full(cqb.shape), full(cos.shape), full(sin.shape),
                full(start.shape),
                pl.BlockSpec((q_lat, 2 * QK_DIM), lambda i, core, *_: (0, core[0] * pairs + i)),
                pl.BlockSpec((KV_LATENT, 2 * KV_DIM), lambda i, core, *_: (0, core[0] * pairs + i)),
            ],
            out_specs=pl.BlockSpec((2 * qb, 2 * VALUE_DIM), lambda i, *_: (0, i)),
            scratch_shapes=[
                pltpu.VMEM((2, tok, 2 * NOPE_DIM), BF16),
                pltpu.VMEM((2, VALUE_DIM, tok), BF16),
                pltpu.VMEM((2, 2 * qb, 2 * NOPE_DIM), BF16),
                pltpu.VMEM((2, VALUE_DIM, qb), F32),
            ]),
        out_shape=jax.ShapeDtypeStruct((2 * qb, heads // 2 * VALUE_DIM), BF16),
        compiler_params=pltpu.CompilerParams(dimension_semantics=("arbitrary",), vmem_limit_bytes=60 * 2 ** 20),
        cost_estimate=pl.CostEstimate(flops=80 * 10 ** 9, bytes_accessed=45 * 10 ** 6, transcendentals=40 * 10 ** 6),
    )(core, lo, mid, blk, ckv, kr, cqa, cqb, cos, sin, start, w_uq, w_ukv)


def tail_body(chips, o_hbm, wo_hbm, wg_hbm, wg2_hbm, wu_hbm, wu2_hbm, wd_hbm, wd2_hbm, g_ref, out_ref,
              obuf, wbuf, acc, xr, yall, hbuf, wg, wu, act, rsr, rss,
              o_sem, w_sem, f_sem, d_sem, xs_sem, xr_sem, as_sem, ar_sem, fs_sem, fr_sem, ss_sem, sr_sem):
    me = lax.axis_index('sp')
    chip, core = me // 2, me % 2
    right, left = (chip + 1) % chips, (chip + chips - 1) % chips
    far = (chip + 2) % chips
    ring = (2 * right + core, 2 * left + core)
    peer = 2 * chip + 1 - core
    src = (left, right)
    nt, kt = acc.shape[0], obuf.shape[1] // wbuf.shape[1]
    nbuf, tk, tn = wbuf.shape
    blk = yall.shape[2]
    half = blk // 2
    depth = kt * tk
    shard = wg_hbm.shape[1]

    def slot_of(q):
        return core * (chips - 1) + (1 - 2 * core) * q

    def remote(s, d, ssem, rsem, dev):
        return pltpu.make_async_remote_copy(src_ref=s, dst_ref=d, send_sem=ssem, recv_sem=rsem,
                                            device_id={'sp': dev}, device_id_type=pl.DeviceIdType.MESH)

    def w_copy(t):
        n, k = t // kt, t % kt
        return pltpu.make_async_copy(
            wo_hbm.at[pl.ds(pl.multiple_of(core * depth + k * tk, tk), tk), pl.ds(pl.multiple_of(n * tn, tn), tn)],
            wbuf.at[t % nbuf], w_sem.at[t % nbuf])

    def o_copy(k):
        cols = pl.ds(pl.multiple_of(k * tk, tk), tk)
        return pltpu.make_async_copy(o_hbm.at[:, cols], obuf.at[:, cols], o_sem.at[k])

    f_copies = [pltpu.make_async_copy(s, d.at[:, pl.ds(c * shard, shard)], f_sem.at[i])
                for i, (s, d, c) in enumerate(((wg_hbm, wg, 0), (wg2_hbm, wg, 1), (wu_hbm, wu, 0), (wu2_hbm, wu, 1)))]
    grain = 256
    width = nt * tn
    n_grain = 2 * shard // grain
    per = obuf.shape[0] // grain
    d_copies = []
    for g in range(n_grain):
        s = wd_hbm if g < n_grain // 2 else wd2_hbm
        d_copies.append(pltpu.make_async_copy(
            s.at[pl.ds((g % (n_grain // 2)) * grain, grain), :],
            obuf.at[pl.ds((g % per) * grain, grain), pl.ds((g // per) * width, width)], d_sem.at[g]))

    for k in range(kt):
        o_copy(k).start()
    for t in range(nbuf - 1):
        w_copy(t).start()

    barrier = pltpu.get_barrier_semaphore()
    for dev in (peer,) + ring:
        pl.semaphore_signal(barrier, inc=1, device_id={'sp': dev}, device_id_type=pl.DeviceIdType.MESH)
    pl.semaphore_wait(barrier, 3)

    own_rows = pl.ds(pl.multiple_of(core * blk, blk), blk)
    peer_rows = pl.ds(pl.multiple_of((1 - core) * blk, blk), blk)

    def x_copy(n):
        return remote(acc.at[n, peer_rows, :], xr.at[n], xs_sem.at[n], xr_sem.at[n], peer)

    def a_copy(d, n, slot):
        return remote(yall.at[slot, n], yall.at[slot, n], as_sem.at[d, n], ar_sem.at[d, n], ring[d])

    def f_copy(d, n, slot):
        rows = pl.ds(d * half, half)
        return remote(yall.at[slot, n, rows, :], yall.at[slot, n, rows, :], fs_sem.at[d, n], fr_sem.at[d, n], ring[d])

    def combine(n):
        x_copy(n).wait_recv()
        yall[chip, n] = (acc[n, own_rows, :] + xr[n]).astype(BF16)
        for d in range(2):
            a_copy(d, n, chip).start()

    def forward(n):
        for d in range(2):
            a_copy(d, n, src[d]).wait_recv()
            f_copy(d, n, src[d]).start()

    def w_step(t, _):
        n, k = t // kt, t % kt

        @pl.when(t + nbuf - 1 < nt * kt)
        def _():
            w_copy(t + nbuf - 1).start()

        @pl.when(t == nbuf)
        def _():
            for c in f_copies:
                c.start()

        @pl.when(n == 0)
        def _():
            o_copy(k).wait()
        w_copy(t).wait()
        prod = jnp.dot(obuf[:, pl.ds(pl.multiple_of(k * tk, tk), tk)], wbuf[t % nbuf], preferred_element_type=F32)

        @pl.when(k == 0)
        def _():
            acc[n] = prod

        @pl.when(k > 0)
        def _():
            acc[n] += prod

        @pl.when(k == kt - 1)
        def _():
            x_copy(n).start()

            @pl.when(n >= 1)
            def _():
                combine(n - 1)

            @pl.when(n >= 3)
            def _():
                forward(n - 3)
        return 0

    lax.fori_loop(0, nt * kt, w_step, 0)
    for c in d_copies:
        c.start()
    combine(nt - 1)
    forward(nt - 3)

    def activate(slot):
        def norm(r, _):
            rows = pl.ds(pl.multiple_of(r * 64, 64), 64)
            ys = [yall[slot, k, rows, :].astype(F32) for k in range(nt)]
            total = sum(jnp.sum(y * y, axis=-1, keepdims=True) for y in ys)
            scale = lax.rsqrt(total * (1.0 / width) + 1e-6)
            for k in range(nt):
                gain = g_ref[:, pl.ds(k * tn, tn)].astype(F32)
                hbuf[k, rows, :] = (ys[k] * scale * gain).astype(BF16)
            return 0
        lax.fori_loop(0, blk // 64, norm, 0)

        def cols(c, _):
            cs = pl.ds(pl.multiple_of(c * 256, 256), 256)
            gate = sum(jnp.dot(hbuf[k], wg[pl.ds(k * tn, tn), cs], preferred_element_type=F32) for k in range(nt))
            up = sum(jnp.dot(hbuf[k], wu[pl.ds(k * tn, tn), cs], preferred_element_type=F32) for k in range(nt))
            act[slot, :, cs] = (jax.nn.silu(gate) * up).astype(BF16)
            return 0
        lax.fori_loop(0, 2 * shard // 256, cols, 0)

    hw = width // 2

    def down(slot, c, d):
        rows = pl.ds(c * half, half)
        return sum(jnp.dot(act[slot, rows, pl.ds(g * grain, grain)],
                           obuf[pl.ds((g % per) * grain, grain), pl.ds((g // per) * width + d * hw, hw)],
                           preferred_element_type=F32) for g in range(n_grain))

    def s_copy(d, s, c):
        src_ref = rss.at[d, c] if s == 0 else rsr.at[d, s - 1, c]
        return remote(src_ref, rsr.at[d, s, c], ss_sem.at[d, s, c], sr_sem.at[d, s, c], ring[d])

    def first():
        for d, q in enumerate((left, right)):
            for c in range(2):
                rss[d, c] = down(slot_of(q), c, d)
                s_copy(d, 0, c).start()

    for c in f_copies:
        c.wait()
    activate(chip)
    forward(nt - 2)
    forward(nt - 1)
    for c in d_copies:
        c.wait()
    activate(left)
    activate(right)

    @pl.when(core == 0)
    def _():
        first()
    for n in range(nt):
        for d in range(2):
            f_copy(d, n, far).wait_recv()
    activate(far)

    @pl.when(core == 1)
    def _():
        first()

    for s, dests in ((1, (far, far)), (2, (right, left))):
        for c in range(2):
            for d in range(2):
                part = down(slot_of(dests[d]), c, d)
                s_copy(d, s - 1, c).wait_recv()
                rsr[d, s - 1, c] = rsr[d, s - 1, c] + part
                s_copy(d, s, c).start()

    mine = slot_of(chip)
    per_half = hw // half
    for c in range(2):
        rows = pl.ds(c * half, half)
        for d in range(2):
            part = down(mine, c, d)
            s_copy(d, 2, c).wait_recv()
            pieces = []
            for col in range(d * hw, (d + 1) * hw, 256):
                pieces.append(yall[mine, col // tn, rows, pl.ds(col % tn, 256)].astype(F32))
            y = jnp.concatenate(pieces, axis=1)
            out_ref[rows, pl.ds(d * hw, hw)] = (y + (rsr[d, 2, c] + part)).astype(BF16)

    for n in range(nt):
        x_copy(n).wait_send()
        for d in range(2):
            a_copy(d, n, chip).wait_send()
            f_copy(d, n, src[d]).wait_send()
    for d in range(2):
        for s in range(3):
            for c in range(2):
                s_copy(d, s, c).wait_send()


def tail(chips, o, w_o, w_gate, w_gate2, w_up, w_up2, w_down, w_down2, g_ffn, nbuf=4, tk=1024, tn=512):
    rows, depth = o.shape
    width = w_o.shape[1]
    shard = w_gate.shape[1]
    blk = rows // 2
    nt, kt = width // tn, depth // tk
    dma = pltpu.SemaphoreType.DMA
    hbm = pl.BlockSpec(memory_space=pl.ANY)
    vmem = pl.BlockSpec(memory_space=pltpu.VMEM)
    return pl.pallas_call(
        functools.partial(tail_body, chips),
        in_specs=[hbm] * 8 + [vmem],
        out_specs=vmem,
        out_shape=jax.ShapeDtypeStruct((blk, width), BF16),
        scratch_shapes=[
            pltpu.VMEM((rows, depth), BF16),
            pltpu.VMEM((nbuf, tk, tn), BF16),
            pltpu.VMEM((nt, rows, tn), F32),
            pltpu.VMEM((nt, blk, tn), F32),
            pltpu.VMEM((chips, nt, blk, tn), BF16),
            pltpu.VMEM((nt, blk, tn), BF16),
            pltpu.VMEM((width, 2 * shard), BF16),
            pltpu.VMEM((width, 2 * shard), BF16),
            pltpu.VMEM((chips, blk, 2 * shard), BF16),
            pltpu.VMEM((2, 3, 2, blk // 2, width // 2), F32),
            pltpu.VMEM((2, 2, blk // 2, width // 2), F32),
            dma((kt,)), dma((nbuf,)), dma((4,)), dma((2 * shard // 256,)),
            dma((nt,)), dma((nt,)), dma((2, nt)), dma((2, nt)), dma((2, nt)), dma((2, nt)),
            dma((2, 3, 2)), dma((2, 3, 2)),
        ],
        compiler_params=pltpu.CompilerParams(collective_id=0, has_side_effects=True,
                                             vmem_limit_bytes=63 * 2 ** 20),
        cost_estimate=pl.CostEstimate(flops=46 * 10 ** 9, bytes_accessed=75 * 10 ** 6, transcendentals=10 ** 6),
    )(o, w_o, w_gate, w_gate2, w_up, w_up2, w_down, w_down2, g_ffn)


def solution(mesh):
    group_size = mesh.shape['sp']
    chips = group_size // 2
    tok_spec = P(('dp', 'sp'), None)
    row_spec = P(('dp', 'sp'))
    full_spec = P()
    col_spec = P(None, 'sp')
    swap = [(d, d ^ 1) for d in range(group_size)]

    def device_fn(x_blk, seg_blk, pos_blk, w_dq, g_q, w_uq, w_dkv, g_kv, w_ukv, w_o, g_ffn, w_gate, w_up, w_down):
        me = lax.axis_index('sp')
        chip, core = me // 2, me % 2
        blk_len = x_blk.shape[0]
        core_arr = core.reshape(1).astype(jnp.int32)

        w_gate2 = lax.ppermute(w_gate, 'sp', swap)
        w_up2 = lax.ppermute(w_up, 'sp', swap)
        w_down2 = lax.ppermute(w_down, 'sp', swap)

        q_lin = jnp.dot(x_blk, w_dq, preferred_element_type=F32)
        c_q = rms_norm(q_lin, g_q).astype(BF16)
        kv_lin = jnp.dot(x_blk, w_dkv, preferred_element_type=F32)
        c_kv = rms_norm(kv_lin[:, :KV_LATENT], g_kv).astype(BF16)
        cosine, sine = rope_tables(pos_blk)
        lo_half, hi_half = kv_lin[:, KV_LATENT:KV_LATENT + ROPE_DIM // 2], kv_lin[:, KV_LATENT + ROPE_DIM // 2:]
        k_rope = jnp.concatenate([lo_half * cosine - hi_half * sine, hi_half * cosine + lo_half * sine],
                                 axis=-1).astype(BF16)
        gather = lambda a: lax.all_gather(a, 'sp', axis=0, tiled=True)
        cq_all, ckv_all, kr_all, pos_all = gather(c_q), gather(c_kv), gather(k_rope), gather(pos_blk)

        blk = jnp.stack([2 * chip, group_size - 1 - 2 * chip]).astype(jnp.int32)
        take = lambda a, b: lax.dynamic_slice_in_dim(a, blk[b] * blk_len, blk_len, axis=0)
        cqa, cqb = take(cq_all, 0), take(cq_all, 1)
        pos_q = jnp.concatenate([take(pos_all, 0), take(pos_all, 1)])
        rows_q = (blk[:, None] * blk_len + jnp.arange(blk_len, dtype=jnp.int32)[None, :]).reshape(-1)
        start = rows_q - pos_q
        cosine, sine = rope_tables(pos_q)
        cos4 = jnp.concatenate([cosine] * 4, axis=1)
        sin4 = jnp.concatenate([-sine, sine, -sine, sine], axis=1)
        lo = start.reshape(2, blk_len)[:, 0] // blk_len
        last = start.reshape(2, blk_len)[:, -1]
        mid = jnp.minimum((last + blk_len - 1) // blk_len, blk)
        mid = jnp.maximum(mid, lo)

        o = attention(core_arr, lo, mid, blk, ckv_all, kr_all, cqa, cqb, cos4, sin4, start[None, :], w_uq, w_ukv)
        return tail(chips, o, w_o, w_gate, w_gate2, w_up, w_up2, w_down, w_down2, g_ffn[None, :])

    return jax.shard_map(device_fn, mesh=mesh, in_specs=(tok_spec, row_spec, row_spec, full_spec, full_spec, full_spec, full_spec, full_spec, full_spec, full_spec, full_spec, col_spec, col_spec, P('sp', None)), out_specs=tok_spec, check_vma=False)
```

```python
import functools
import jax
import jax.numpy as jnp
from jax import lax
from jax.experimental import pallas as pl
from jax.experimental.pallas import tpu as pltpu
from jax.sharding import PartitionSpec as P

NOPE_DIM = 128
ROPE_DIM = 64
VALUE_DIM = 128
KV_LATENT = 512
QK_DIM = NOPE_DIM + ROPE_DIM
KV_DIM = NOPE_DIM + VALUE_DIM
SCORE_SCALE = QK_DIM ** -0.5
LOG2E = 1.4426950408889634
NEG = -2.0e38
F32 = jnp.float32
BF16 = jnp.bfloat16


def rms_norm(vec_in, gain_vec):
    mean_sq = jnp.mean(vec_in * vec_in, axis=-1, keepdims=True)
    return vec_in * lax.rsqrt(mean_sq + 1e-6) * gain_vec.astype(F32)


def rope_tables(positions):
    half_dim = ROPE_DIM // 2
    inv_freq = 10000.0 ** (-jnp.arange(half_dim, dtype=F32) / half_dim)
    angles = positions.astype(F32)[..., None] * inv_freq
    return jnp.cos(angles), jnp.sin(angles)


def attn_body(core_ref, lo_ref, mid_ref, blk_ref, ckv_ref, kr_ref, cqa_ref, cqb_ref, cos_ref, sin_ref, start_ref,
              wuq_ref, wukv_ref, o_ref, kcat, vt, qcat, sbuf, mbuf, acc, *, kb):
    i = pl.program_id(0)
    tok = ckv_ref.shape[0]
    qb = cqa_ref.shape[0]
    cur, prev = i % 2, (i + 1) % 2

    @pl.when(i == 0)
    def _():
        kr = kr_ref[...]
        pad = jnp.concatenate([kr, jnp.zeros_like(kr)], axis=1)
        for h in range(2):
            kcat[h, :, NOPE_DIM:] = pad

    for r in range(tok // 512):
        rows = pl.ds(r * 512, 512)
        e = jnp.dot(ckv_ref[rows, :], wukv_ref[...], preferred_element_type=F32).astype(BF16)
        for h in range(2):
            kcat[h, rows, :NOPE_DIM] = e[:, KV_DIM * h:KV_DIM * h + NOPE_DIM]
            vt[cur, h, :, rows] = e[:, KV_DIM * h + NOPE_DIM:KV_DIM * (h + 1)].T

    for b, cq in enumerate((cqa_ref, cqb_ref)):
        rows = pl.ds(b * qb, qb)
        q = jnp.dot(cq[...], wuq_ref[...], preferred_element_type=F32)
        q_r = jnp.concatenate([q[:, NOPE_DIM:QK_DIM], q[:, QK_DIM + NOPE_DIM:]], axis=1)
        lane = lax.broadcasted_iota(jnp.int32, q_r.shape, 1)
        lo_half = (lane % ROPE_DIM) < (ROPE_DIM // 2)
        swapped = jnp.where(lo_half, pltpu.roll(q_r, 2 * ROPE_DIM - ROPE_DIM // 2, 1), pltpu.roll(q_r, ROPE_DIM // 2, 1))
        q_r = (q_r * cos_ref[rows, :] + swapped * sin_ref[rows, :]).astype(BF16)
        zero = jnp.zeros((qb, ROPE_DIM), BF16)
        for h in range(2):
            qcat[b, h, :, :NOPE_DIM] = q[:, QK_DIM * h:QK_DIM * h + NOPE_DIM].astype(BF16)
            qcat[b, h, :, NOPE_DIM:] = jnp.concatenate([q_r[:, ROPE_DIM * h:ROPE_DIM * (h + 1)], zero], axis=1)

    def q_block(b, _):
        t0 = blk_ref[b] * qb

        def step(j, carry, masked):
            k0 = pl.multiple_of(j * kb, kb)
            krows = pl.ds(k0, kb)
            new = []
            for h in range(2):
                m, l = carry[2 * h], carry[2 * h + 1]
                s = lax.dot_general(kcat[h, krows, :], qcat[b, h], (((1,), (1,)), ((), ())),
                                    preferred_element_type=F32)
                s = s * (SCORE_SCALE * LOG2E)
                if masked:
                    r = k0 + lax.broadcasted_iota(jnp.int32, s.shape, 0)
                    t = t0 + lax.broadcasted_iota(jnp.int32, s.shape, 1)
                    s = jnp.where((r <= t) & (r >= start_ref[b]), s, NEG)
                m = jnp.maximum(m, jnp.max(s.reshape(kb // 8, 8, qb), axis=0))
                p = jnp.exp2(sbuf[prev, b, h, krows, :] - mbuf[prev, b, h])
                l = l + jnp.sum(p.reshape(kb // 8, 8, qb), axis=0)
                acc[h] += jnp.dot(vt[prev, h, :, krows], p.astype(BF16), preferred_element_type=F32)
                sbuf[cur, b, h, krows, :] = s
                new += [m, l]
            return tuple(new)

        acc[...] = jnp.zeros_like(acc)
        init = (jnp.full((8, qb), NEG, F32), jnp.zeros((8, qb), F32)) * 2
        carry = lax.fori_loop(lo_ref[b], mid_ref[b], functools.partial(step, masked=True), init)
        last = (t0 + qb - 1) // kb
        carry = lax.fori_loop(mid_ref[b], last, functools.partial(step, masked=False), carry)
        carry = step(last, carry, True)
        for h in range(2):
            mbuf[cur, b, h] = jnp.max(carry[2 * h], axis=0, keepdims=True)
            l = jnp.sum(carry[2 * h + 1], axis=0, keepdims=True)
            o = (acc[h] * (1.0 / l)).astype(BF16)
            o_ref[pl.ds(pl.multiple_of(b * qb, qb), qb), VALUE_DIM * h:VALUE_DIM * (h + 1)] = o.T
        return 0

    lax.fori_loop(0, 2, q_block, 0)


def attention(core, lo, mid, blk, ckv, kr, cqa, cqb, cos, sin, start, w_uq, w_ukv, kb):
    tok = ckv.shape[0]
    qb, q_lat = cqa.shape
    heads = w_uq.shape[1] // QK_DIM
    pairs = heads // 4
    full = lambda shape: pl.BlockSpec(shape, lambda i, *_: (0,) * len(shape), pipeline_mode=pl.Buffered(1))
    group = lambda i, core: core[0] * pairs + jnp.minimum(i, pairs - 1)
    return pl.pallas_call(
        functools.partial(attn_body, kb=kb),
        grid_spec=pltpu.PrefetchScalarGridSpec(
            num_scalar_prefetch=4,
            grid=(pairs + 1,),
            in_specs=[
                full(ckv.shape), full(kr.shape), full(cqa.shape), full(cqb.shape), full(cos.shape), full(sin.shape),
                full(start.shape),
                pl.BlockSpec((q_lat, 2 * QK_DIM), lambda i, core, *_: (0, group(i, core))),
                pl.BlockSpec((KV_LATENT, 2 * KV_DIM), lambda i, core, *_: (0, group(i, core))),
            ],
            out_specs=pl.BlockSpec((2 * qb, 2 * VALUE_DIM), lambda i, *_: (0, jnp.maximum(i - 1, 0))),
            scratch_shapes=[
                pltpu.VMEM((2, tok, 2 * NOPE_DIM), BF16),
                pltpu.VMEM((2, 2, VALUE_DIM, tok), BF16),
                pltpu.VMEM((2, 2, qb, 2 * NOPE_DIM), BF16),
                pltpu.VMEM((2, 2, 2, tok, qb), F32),
                pltpu.VMEM((2, 2, 2, 1, qb), F32),
                pltpu.VMEM((2, VALUE_DIM, qb), F32),
            ]),
        out_shape=jax.ShapeDtypeStruct((2 * qb, heads // 2 * VALUE_DIM), BF16),
        compiler_params=pltpu.CompilerParams(dimension_semantics=("arbitrary",), vmem_limit_bytes=62 * 2 ** 20),
        cost_estimate=pl.CostEstimate(flops=80 * 10 ** 9, bytes_accessed=45 * 10 ** 6, transcendentals=40 * 10 ** 6),
    )(core, lo, mid, blk, ckv, kr, cqa, cqb, cos, sin, start, w_uq, w_ukv)


def tail_body(chips, o_hbm, wo_hbm, wg_hbm, wg2_hbm, wu_hbm, wu2_hbm, wd_hbm, wd2_hbm, g_ref, out_ref,
              obuf, wbuf, acc, xr, yall, hbuf, wg, wu, act, rsr, rss,
              o_sem, w_sem, f_sem, d_sem, xs_sem, xr_sem, as_sem, ar_sem, fs_sem, fr_sem, ss_sem, sr_sem):
    me = lax.axis_index('sp')
    chip, core = me // 2, me % 2
    right, left = (chip + 1) % chips, (chip + chips - 1) % chips
    far = (chip + 2) % chips
    ring = (2 * right + core, 2 * left + core)
    peer = 2 * chip + 1 - core
    src = (left, right)
    nt, kt = acc.shape[0], obuf.shape[1] // wbuf.shape[1]
    nbuf, tk, tn = wbuf.shape
    blk = yall.shape[2]
    half = blk // 2
    depth = kt * tk
    shard = wg_hbm.shape[1]

    def slot_of(q):
        return core * (chips - 1) + (1 - 2 * core) * q

    def remote(s, d, ssem, rsem, dev):
        return pltpu.make_async_remote_copy(src_ref=s, dst_ref=d, send_sem=ssem, recv_sem=rsem,
                                            device_id={'sp': dev}, device_id_type=pl.DeviceIdType.MESH)

    def w_copy(t):
        n, k = t // kt, t % kt
        return pltpu.make_async_copy(
            wo_hbm.at[pl.ds(pl.multiple_of(core * depth + k * tk, tk), tk), pl.ds(pl.multiple_of(n * tn, tn), tn)],
            wbuf.at[t % nbuf], w_sem.at[t % nbuf])

    def o_copy(k):
        cols = pl.ds(pl.multiple_of(k * tk, tk), tk)
        return pltpu.make_async_copy(o_hbm.at[:, cols], obuf.at[:, cols], o_sem.at[k])

    f_copies = [pltpu.make_async_copy(s, d.at[:, pl.ds(c * shard, shard)], f_sem.at[i])
                for i, (s, d, c) in enumerate(((wg_hbm, wg, 0), (wg2_hbm, wg, 1), (wu_hbm, wu, 0), (wu2_hbm, wu, 1)))]
    grain = 256
    width = nt * tn
    n_grain = 2 * shard // grain
    per = obuf.shape[0] // grain
    d_copies = []
    for g in range(n_grain):
        s = wd_hbm if g < n_grain // 2 else wd2_hbm
        d_copies.append(pltpu.make_async_copy(
            s.at[pl.ds((g % (n_grain // 2)) * grain, grain), :],
            obuf.at[pl.ds((g % per) * grain, grain), pl.ds((g // per) * width, width)], d_sem.at[g]))

    for k in range(kt):
        o_copy(k).start()
    for t in range(nbuf - 1):
        w_copy(t).start()

    barrier = pltpu.get_barrier_semaphore()
    for dev in (peer,) + ring:
        pl.semaphore_signal(barrier, inc=1, device_id={'sp': dev}, device_id_type=pl.DeviceIdType.MESH)
    pl.semaphore_wait(barrier, 3)

    own_rows = pl.ds(pl.multiple_of(core * blk, blk), blk)
    peer_rows = pl.ds(pl.multiple_of((1 - core) * blk, blk), blk)

    def x_copy(n):
        return remote(acc.at[n, peer_rows, :], xr.at[n], xs_sem.at[n], xr_sem.at[n], peer)

    def a_copy(d, n, slot):
        return remote(yall.at[slot, n], yall.at[slot, n], as_sem.at[d, n], ar_sem.at[d, n], ring[d])

    def f_copy(d, n, slot):
        rows = pl.ds(d * half, half)
        return remote(yall.at[slot, n, rows, :], yall.at[slot, n, rows, :], fs_sem.at[d, n], fr_sem.at[d, n], ring[d])

    def combine(n):
        x_copy(n).wait_recv()
        yall[chip, n] = (acc[n, own_rows, :] + xr[n]).astype(BF16)
        for d in range(2):
            a_copy(d, n, chip).start()

    def forward(n):
        for d in range(2):
            a_copy(d, n, src[d]).wait_recv()
            f_copy(d, n, src[d]).start()

    def w_step(t, _):
        n, k = t // kt, t % kt

        @pl.when(t + nbuf - 1 < nt * kt)
        def _():
            w_copy(t + nbuf - 1).start()

        @pl.when(t == nbuf)
        def _():
            for c in f_copies:
                c.start()

        @pl.when(n == 0)
        def _():
            o_copy(k).wait()
        w_copy(t).wait()
        prod = jnp.dot(obuf[:, pl.ds(pl.multiple_of(k * tk, tk), tk)], wbuf[t % nbuf], preferred_element_type=F32)

        @pl.when(k == 0)
        def _():
            acc[n] = prod

        @pl.when(k > 0)
        def _():
            acc[n] += prod

        @pl.when(k == kt - 1)
        def _():
            x_copy(n).start()

            @pl.when(n >= 1)
            def _():
                combine(n - 1)

            @pl.when(n >= 3)
            def _():
                forward(n - 3)
        return 0

    lax.fori_loop(0, nt * kt, w_step, 0)
    for c in d_copies:
        c.start()
    combine(nt - 1)
    forward(nt - 3)

    def activate(slot):
        def norm(r, _):
            rows = pl.ds(pl.multiple_of(r * 64, 64), 64)
            ys = [yall[slot, k, rows, :].astype(F32) for k in range(nt)]
            total = sum(jnp.sum(y * y, axis=-1, keepdims=True) for y in ys)
            scale = lax.rsqrt(total * (1.0 / width) + 1e-6)
            for k in range(nt):
                gain = g_ref[:, pl.ds(k * tn, tn)].astype(F32)
                hbuf[k, rows, :] = (ys[k] * scale * gain).astype(BF16)
            return 0
        lax.fori_loop(0, blk // 64, norm, 0)

        def cols(c, _):
            cs = pl.ds(pl.multiple_of(c * 256, 256), 256)
            gate = sum(jnp.dot(hbuf[k], wg[pl.ds(k * tn, tn), cs], preferred_element_type=F32) for k in range(nt))
            up = sum(jnp.dot(hbuf[k], wu[pl.ds(k * tn, tn), cs], preferred_element_type=F32) for k in range(nt))
            act[slot, :, cs] = (jax.nn.silu(gate) * up).astype(BF16)
            return 0
        lax.fori_loop(0, 2 * shard // 256, cols, 0)

    hw = width // 2

    def down(slot, c, d):
        rows = pl.ds(c * half, half)
        return sum(jnp.dot(act[slot, rows, pl.ds(g * grain, grain)],
                           obuf[pl.ds((g % per) * grain, grain), pl.ds((g // per) * width + d * hw, hw)],
                           preferred_element_type=F32) for g in range(n_grain))

    def s_copy(d, s, c):
        src_ref = rss.at[d, c] if s == 0 else rsr.at[d, s - 1, c]
        return remote(src_ref, rsr.at[d, s, c], ss_sem.at[d, s, c], sr_sem.at[d, s, c], ring[d])

    def first():
        for d, q in enumerate((left, right)):
            for c in range(2):
                rss[d, c] = down(slot_of(q), c, d)
                s_copy(d, 0, c).start()

    for c in f_copies:
        c.wait()
    activate(chip)
    forward(nt - 2)
    forward(nt - 1)
    for c in d_copies:
        c.wait()
    activate(left)
    activate(right)

    @pl.when(core == 0)
    def _():
        first()
    for n in range(nt):
        for d in range(2):
            f_copy(d, n, far).wait_recv()
    activate(far)

    @pl.when(core == 1)
    def _():
        first()

    for s, dests in ((1, (far, far)), (2, (right, left))):
        for c in range(2):
            for d in range(2):
                part = down(slot_of(dests[d]), c, d)
                s_copy(d, s - 1, c).wait_recv()
                rsr[d, s - 1, c] = rsr[d, s - 1, c] + part
                s_copy(d, s, c).start()

    mine = slot_of(chip)
    per_half = hw // half
    for c in range(2):
        rows = pl.ds(c * half, half)
        for d in range(2):
            part = down(mine, c, d)
            s_copy(d, 2, c).wait_recv()
            pieces = []
            for col in range(d * hw, (d + 1) * hw, 256):
                pieces.append(yall[mine, col // tn, rows, pl.ds(col % tn, 256)].astype(F32))
            y = jnp.concatenate(pieces, axis=1)
            out_ref[rows, pl.ds(d * hw, hw)] = (y + (rsr[d, 2, c] + part)).astype(BF16)

    for n in range(nt):
        x_copy(n).wait_send()
        for d in range(2):
            a_copy(d, n, chip).wait_send()
            f_copy(d, n, src[d]).wait_send()
    for d in range(2):
        for s in range(3):
            for c in range(2):
                s_copy(d, s, c).wait_send()


def tail(chips, o, w_o, w_gate, w_gate2, w_up, w_up2, w_down, w_down2, g_ffn, nbuf=4, tk=1024, tn=512):
    rows, depth = o.shape
    width = w_o.shape[1]
    shard = w_gate.shape[1]
    blk = rows // 2
    nt, kt = width // tn, depth // tk
    dma = pltpu.SemaphoreType.DMA
    hbm = pl.BlockSpec(memory_space=pl.ANY)
    vmem = pl.BlockSpec(memory_space=pltpu.VMEM)
    return pl.pallas_call(
        functools.partial(tail_body, chips),
        in_specs=[hbm] * 8 + [vmem],
        out_specs=vmem,
        out_shape=jax.ShapeDtypeStruct((blk, width), BF16),
        scratch_shapes=[
            pltpu.VMEM((rows, depth), BF16),
            pltpu.VMEM((nbuf, tk, tn), BF16),
            pltpu.VMEM((nt, rows, tn), F32),
            pltpu.VMEM((nt, blk, tn), F32),
            pltpu.VMEM((chips, nt, blk, tn), BF16),
            pltpu.VMEM((nt, blk, tn), BF16),
            pltpu.VMEM((width, 2 * shard), BF16),
            pltpu.VMEM((width, 2 * shard), BF16),
            pltpu.VMEM((chips, blk, 2 * shard), BF16),
            pltpu.VMEM((2, 3, 2, blk // 2, width // 2), F32),
            pltpu.VMEM((2, 2, blk // 2, width // 2), F32),
            dma((kt,)), dma((nbuf,)), dma((4,)), dma((2 * shard // 256,)),
            dma((nt,)), dma((nt,)), dma((2, nt)), dma((2, nt)), dma((2, nt)), dma((2, nt)),
            dma((2, 3, 2)), dma((2, 3, 2)),
        ],
        compiler_params=pltpu.CompilerParams(collective_id=0, has_side_effects=True,
                                             vmem_limit_bytes=63 * 2 ** 20),
        cost_estimate=pl.CostEstimate(flops=46 * 10 ** 9, bytes_accessed=75 * 10 ** 6, transcendentals=10 ** 6),
    )(o, w_o, w_gate, w_gate2, w_up, w_up2, w_down, w_down2, g_ffn)


def solution(mesh):
    group_size = mesh.shape['sp']
    chips = group_size // 2
    tok_spec = P(('dp', 'sp'), None)
    row_spec = P(('dp', 'sp'))
    full_spec = P()
    col_spec = P(None, 'sp')
    swap = [(d, d ^ 1) for d in range(group_size)]

    def device_fn(x_blk, seg_blk, pos_blk, w_dq, g_q, w_uq, w_dkv, g_kv, w_ukv, w_o, g_ffn, w_gate, w_up, w_down):
        me = lax.axis_index('sp')
        chip, core = me // 2, me % 2
        blk_len = x_blk.shape[0]
        core_arr = core.reshape(1).astype(jnp.int32)

        w_gate2 = lax.ppermute(w_gate, 'sp', swap)
        w_up2 = lax.ppermute(w_up, 'sp', swap)
        w_down2 = lax.ppermute(w_down, 'sp', swap)

        q_lin = jnp.dot(x_blk, w_dq, preferred_element_type=F32)
        c_q = rms_norm(q_lin, g_q).astype(BF16)
        kv_lin = jnp.dot(x_blk, w_dkv, preferred_element_type=F32)
        c_kv = rms_norm(kv_lin[:, :KV_LATENT], g_kv).astype(BF16)
        cosine, sine = rope_tables(pos_blk)
        lo_half, hi_half = kv_lin[:, KV_LATENT:KV_LATENT + ROPE_DIM // 2], kv_lin[:, KV_LATENT + ROPE_DIM // 2:]
        k_rope = jnp.concatenate([lo_half * cosine - hi_half * sine, hi_half * cosine + lo_half * sine],
                                 axis=-1).astype(BF16)
        gather = lambda a: lax.all_gather(a, 'sp', axis=0, tiled=True)
        cq_all, ckv_all, kr_all, pos_all = gather(c_q), gather(c_kv), gather(k_rope), gather(pos_blk)

        blk = jnp.stack([2 * chip, group_size - 1 - 2 * chip]).astype(jnp.int32)
        take = lambda a, b: lax.dynamic_slice_in_dim(a, blk[b] * blk_len, blk_len, axis=0)
        cqa, cqb = take(cq_all, 0), take(cq_all, 1)
        pos_q = jnp.concatenate([take(pos_all, 0), take(pos_all, 1)])
        rows_q = (blk[:, None] * blk_len + jnp.arange(blk_len, dtype=jnp.int32)[None, :]).reshape(-1)
        start = rows_q - pos_q
        cosine, sine = rope_tables(pos_q)
        cos4 = jnp.concatenate([cosine] * 4, axis=1)
        sin4 = jnp.concatenate([-sine, sine, -sine, sine], axis=1)
        kb = 2 * blk_len
        start = start.reshape(2, 1, blk_len)
        lo = start[:, 0, 0] // kb
        last = (blk * blk_len + blk_len - 1) // kb
        mid = jnp.maximum(jnp.minimum((start[:, 0, -1] + kb - 1) // kb, last), lo)

        o = attention(core_arr, lo, mid, blk, ckv_all, kr_all, cqa, cqb, cos4, sin4, start, w_uq, w_ukv, kb)
        return tail(chips, o, w_o, w_gate, w_gate2, w_up, w_up2, w_down, w_down2, g_ffn[None, :])

    return jax.shard_map(device_fn, mesh=mesh, in_specs=(tok_spec, row_spec, row_spec, full_spec, full_spec, full_spec, full_spec, full_spec, full_spec, full_spec, full_spec, col_spec, col_spec, P('sp', None)), out_specs=tok_spec, check_vma=False)
```

```python
import functools
import jax
import jax.numpy as jnp
from jax import lax
from jax.experimental import pallas as pl
from jax.experimental.pallas import tpu as pltpu
from jax.sharding import PartitionSpec as P

NOPE_DIM = 128
ROPE_DIM = 64
VALUE_DIM = 128
KV_LATENT = 512
QK_DIM = NOPE_DIM + ROPE_DIM
KV_DIM = NOPE_DIM + VALUE_DIM
SCORE_SCALE = QK_DIM ** -0.5
LOG2E = 1.4426950408889634
NEG = -2.0e38
F32 = jnp.float32
BF16 = jnp.bfloat16


def rms_norm(vec_in, gain_vec):
    mean_sq = jnp.mean(vec_in * vec_in, axis=-1, keepdims=True)
    return vec_in * lax.rsqrt(mean_sq + 1e-6) * gain_vec.astype(F32)


def rope_tables(positions):
    half_dim = ROPE_DIM // 2
    inv_freq = 10000.0 ** (-jnp.arange(half_dim, dtype=F32) / half_dim)
    angles = positions.astype(F32)[..., None] * inv_freq
    return jnp.cos(angles), jnp.sin(angles)


def latent_body(chips, x_ref, wdq_ref, gq_ref, wdkv_ref, gkv_ref, tab_ref,
                kvr_ref, cqa_ref, cqb_ref, taba_ref, tabb_ref, cq_s,
                rs_sem, rr_sem, fs_sem, fr_sem, ps_sem, pr_sem, qs_sem, qr_sem):
    me = lax.axis_index('sp')
    chip, core = me // 2, me % 2
    right, left = (chip + 1) % chips, (chip + chips - 1) % chips
    far = (chip + 2) % chips
    ring = (2 * right + core, 2 * left + core)
    src = (left, right)
    peer = 2 * chip + 1 - core
    mirror = chips - 1 - chip
    blk = x_ref.shape[0]
    half = blk // 2

    def remote(s, d, ssem, rsem, dev):
        return pltpu.make_async_remote_copy(src_ref=s, dst_ref=d, send_sem=ssem, recv_sem=rsem,
                                            device_id={'sp': dev}, device_id_type=pl.DeviceIdType.MESH)

    barrier = pltpu.get_barrier_semaphore()
    for dev in (peer,) + ring + (2 * mirror + 1 - core,):
        pl.semaphore_signal(barrier, inc=1, device_id={'sp': dev}, device_id_type=pl.DeviceIdType.MESH)

    def block(c, k, part=None):
        start = (2 * c + k) * blk
        if part is None:
            return kvr_ref.at[pl.ds(pl.multiple_of(start, blk), blk), :]
        return kvr_ref.at[pl.ds(pl.multiple_of(start + part * half, half), half), :]

    def ring_copy(d, c):
        return remote(block(c, core), block(c, core), rs_sem.at[d], rr_sem.at[d], ring[d])

    def fwd_copy(d, c):
        return remote(block(c, core, d), block(c, core, d), fs_sem.at[d], fr_sem.at[d], ring[d])

    def peer_copy(i, c, k, part=None):
        return remote(block(c, k, part), block(c, k, part), ps_sem.at[i], pr_sem.at[i], peer)

    x = x_ref[...]
    lat = wdkv_ref.shape[1] - ROPE_DIM
    kv = jnp.dot(x, wdkv_ref[:, :lat], preferred_element_type=F32)
    c_kv = rms_norm(kv, gkv_ref[...]).astype(BF16)
    kr = jnp.dot(x, wdkv_ref[:, lat:], preferred_element_type=F32)
    hd = ROPE_DIM // 2
    cosine, sine = tab_ref[:, :hd], tab_ref[:, hd:2 * hd]
    lo_half, hi_half = kr[:, :hd], kr[:, hd:]
    kr = jnp.concatenate([lo_half * cosine - hi_half * sine, hi_half * cosine + lo_half * sine,
                          jnp.zeros((blk, ROPE_DIM), F32)], axis=1)
    own = pl.ds(pl.multiple_of(me * blk, blk), blk)
    kvr_ref[own, :lat] = c_kv
    kvr_ref[own, lat:] = kr.astype(BF16)

    pl.semaphore_wait(barrier, 4)
    for d in range(2):
        ring_copy(d, chip).start()
    peer_copy(0, chip, core).start()

    cq_s[...] = rms_norm(jnp.dot(x, wdq_ref[...], preferred_element_type=F32), gq_ref[...]).astype(BF16)
    pairs = ((0, cq_s, cqa_ref, cqb_ref), (1, tab_ref, taba_ref, tabb_ref))

    def qa_copy(i, s, a):
        return remote(s, a, qs_sem.at[i], qr_sem.at[i], peer)

    def qb_copy(i, s, b, k):
        return remote(s, b, qs_sem.at[2 * k + i], qr_sem.at[2 + i], 2 * mirror + k)

    @pl.when(core == 0)
    def _():
        for i, s, a, b in pairs:
            qa_copy(i, s, a).start()
        cqa_ref[...] = cq_s[...]
        taba_ref[...] = tab_ref[...]

    @pl.when(core == 1)
    def _():
        for i, s, a, b in pairs:
            for k in range(2):
                qb_copy(i, s, b, k).start()

    for d in range(2):
        ring_copy(d, src[d]).wait_recv()
        fwd_copy(d, src[d]).start()
        peer_copy(1 + d, src[d], core).start()
    for d in range(2):
        fwd_copy(d, far).wait_recv()
        peer_copy(3 + d, far, core, d).start()

    for i, s, a, b in pairs:
        qb_copy(i, s, b, 0).wait_recv()

    @pl.when(core == 1)
    def _():
        for i, s, a, b in pairs:
            qa_copy(i, s, a).wait_recv()
            for k in range(2):
                qb_copy(i, s, b, k).wait_send()

    @pl.when(core == 0)
    def _():
        for i, s, a, b in pairs:
            qa_copy(i, s, a).wait_send()

    other = 1 - core
    waits = ((0, chip, None), (1, left, None), (2, right, None), (3, far, 0), (4, far, 1))
    for i, c, part in waits:
        peer_copy(i, c, other, part).wait_recv()
    for i, c, part in waits:
        peer_copy(i, c, core, part).wait_send()
    for d in range(2):
        ring_copy(d, chip).wait_send()
        fwd_copy(d, src[d]).wait_send()


def latents(chips, x, w_dq, g_q, w_dkv, g_kv, tab):
    blk = x.shape[0]
    lat = w_dkv.shape[1] - ROPE_DIM
    tok = 2 * chips * blk
    dma = pltpu.SemaphoreType.DMA
    vmem = pl.BlockSpec(memory_space=pltpu.VMEM)
    shape = jax.ShapeDtypeStruct
    return pl.pallas_call(
        functools.partial(latent_body, chips),
        in_specs=[vmem] * 6,
        out_specs=[vmem] * 5,
        out_shape=[shape((tok, lat + 2 * ROPE_DIM), BF16), shape((blk, w_dq.shape[1]), BF16),
                   shape((blk, w_dq.shape[1]), BF16), shape(tab.shape, F32), shape(tab.shape, F32)],
        scratch_shapes=[pltpu.VMEM((blk, w_dq.shape[1]), BF16)] + [dma((2,))] * 4 + [dma((5,))] * 2 + [dma((4,))] * 2,
        compiler_params=pltpu.CompilerParams(collective_id=1, has_side_effects=True, vmem_limit_bytes=40 * 2 ** 20),
        cost_estimate=pl.CostEstimate(flops=2 * 10 ** 9, bytes_accessed=10 ** 7, transcendentals=0),
    )(x, w_dq, g_q[None, :], w_dkv, g_kv[None, :], tab)


def attn_body(core_ref, lo_ref, mid_ref, blk_ref, kvr_ref, cqa_ref, cqb_ref, cos_ref, sin_ref, start_ref,
              wuq_ref, wukv_ref, o_ref, kcat, vt, qcat, sbuf, mbuf, acc, *, kb):
    i = pl.program_id(0)
    tok = kvr_ref.shape[0]
    qb = cqa_ref.shape[0]
    cur, prev = i % 2, (i + 1) % 2

    @pl.when(i == 0)
    def _():
        for h in range(2):
            kcat[h, :, NOPE_DIM:] = kvr_ref[:, KV_LATENT:]

    for r in range(tok // 512):
        rows = pl.ds(r * 512, 512)
        e = jnp.dot(kvr_ref[rows, :KV_LATENT], wukv_ref[...], preferred_element_type=F32).astype(BF16)
        for h in range(2):
            kcat[h, rows, :NOPE_DIM] = e[:, KV_DIM * h:KV_DIM * h + NOPE_DIM]
            vt[cur, h, :, rows] = e[:, KV_DIM * h + NOPE_DIM:KV_DIM * (h + 1)].T

    for b, cq in enumerate((cqa_ref, cqb_ref)):
        rows = pl.ds(b * qb, qb)
        q = jnp.dot(cq[...], wuq_ref[...], preferred_element_type=F32)
        q_r = jnp.concatenate([q[:, NOPE_DIM:QK_DIM], q[:, QK_DIM + NOPE_DIM:]], axis=1)
        lane = lax.broadcasted_iota(jnp.int32, q_r.shape, 1)
        lo_half = (lane % ROPE_DIM) < (ROPE_DIM // 2)
        swapped = jnp.where(lo_half, pltpu.roll(q_r, 2 * ROPE_DIM - ROPE_DIM // 2, 1), pltpu.roll(q_r, ROPE_DIM // 2, 1))
        q_r = (q_r * cos_ref[rows, :] + swapped * sin_ref[rows, :]).astype(BF16)
        zero = jnp.zeros((qb, ROPE_DIM), BF16)
        for h in range(2):
            qcat[b, h, :, :NOPE_DIM] = q[:, QK_DIM * h:QK_DIM * h + NOPE_DIM].astype(BF16)
            qcat[b, h, :, NOPE_DIM:] = jnp.concatenate([q_r[:, ROPE_DIM * h:ROPE_DIM * (h + 1)], zero], axis=1)

    def q_block(b, _):
        t0 = blk_ref[b] * qb

        def step(j, carry, masked):
            k0 = pl.multiple_of(j * kb, kb)
            krows = pl.ds(k0, kb)
            new = []
            for h in range(2):
                m, l = carry[2 * h], carry[2 * h + 1]
                s = lax.dot_general(kcat[h, krows, :], qcat[b, h], (((1,), (1,)), ((), ())),
                                    preferred_element_type=F32)
                s = s * (SCORE_SCALE * LOG2E)
                if masked:
                    r = k0 + lax.broadcasted_iota(jnp.int32, s.shape, 0)
                    t = t0 + lax.broadcasted_iota(jnp.int32, s.shape, 1)
                    s = jnp.where((r <= t) & (r >= start_ref[b]), s, NEG)
                m = jnp.maximum(m, jnp.max(s.reshape(kb // 8, 8, qb), axis=0))
                p = jnp.exp2(sbuf[prev, b, h, krows, :] - mbuf[prev, b, h])
                l = l + jnp.sum(p.reshape(kb // 8, 8, qb), axis=0)
                acc[h] += jnp.dot(vt[prev, h, :, krows], p.astype(BF16), preferred_element_type=F32)
                sbuf[cur, b, h, krows, :] = s
                new += [m, l]
            return tuple(new)

        acc[...] = jnp.zeros_like(acc)
        init = (jnp.full((8, qb), NEG, F32), jnp.zeros((8, qb), F32)) * 2
        carry = lax.fori_loop(lo_ref[b], mid_ref[b], functools.partial(step, masked=True), init)
        last = (t0 + qb - 1) // kb
        carry = lax.fori_loop(mid_ref[b], last, functools.partial(step, masked=False), carry)
        carry = step(last, carry, True)
        for h in range(2):
            mbuf[cur, b, h] = jnp.max(carry[2 * h], axis=0, keepdims=True)
            l = jnp.sum(carry[2 * h + 1], axis=0, keepdims=True)
            o = (acc[h] * (1.0 / l)).astype(BF16)
            o_ref[pl.ds(pl.multiple_of(b * qb, qb), qb), VALUE_DIM * h:VALUE_DIM * (h + 1)] = o.T
        return 0

    lax.fori_loop(0, 2, q_block, 0)


def attention(core, lo, mid, blk, kvr, cqa, cqb, cos, sin, start, w_uq, w_ukv, kb):
    tok = kvr.shape[0]
    qb, q_lat = cqa.shape
    heads = w_uq.shape[1] // QK_DIM
    pairs = heads // 4
    full = lambda shape: pl.BlockSpec(shape, lambda i, *_: (0,) * len(shape), pipeline_mode=pl.Buffered(1))
    group = lambda i, core: core[0] * pairs + jnp.minimum(i, pairs - 1)
    return pl.pallas_call(
        functools.partial(attn_body, kb=kb),
        grid_spec=pltpu.PrefetchScalarGridSpec(
            num_scalar_prefetch=4,
            grid=(pairs + 1,),
            in_specs=[
                full(kvr.shape), full(cqa.shape), full(cqb.shape), full(cos.shape), full(sin.shape),
                full(start.shape),
                pl.BlockSpec((q_lat, 2 * QK_DIM), lambda i, core, *_: (0, group(i, core))),
                pl.BlockSpec((KV_LATENT, 2 * KV_DIM), lambda i, core, *_: (0, group(i, core))),
            ],
            out_specs=pl.BlockSpec((2 * qb, 2 * VALUE_DIM), lambda i, *_: (0, jnp.maximum(i - 1, 0))),
            scratch_shapes=[
                pltpu.VMEM((2, tok, 2 * NOPE_DIM), BF16),
                pltpu.VMEM((2, 2, VALUE_DIM, tok), BF16),
                pltpu.VMEM((2, 2, qb, 2 * NOPE_DIM), BF16),
                pltpu.VMEM((2, 2, 2, tok, qb), F32),
                pltpu.VMEM((2, 2, 2, 1, qb), F32),
                pltpu.VMEM((2, VALUE_DIM, qb), F32),
            ]),
        out_shape=jax.ShapeDtypeStruct((2 * qb, heads // 2 * VALUE_DIM), BF16),
        compiler_params=pltpu.CompilerParams(dimension_semantics=("arbitrary",), vmem_limit_bytes=62 * 2 ** 20),
        cost_estimate=pl.CostEstimate(flops=80 * 10 ** 9, bytes_accessed=45 * 10 ** 6, transcendentals=40 * 10 ** 6),
    )(core, lo, mid, blk, kvr, cqa, cqb, cos, sin, start, w_uq, w_ukv)


def tail_body(chips, o_hbm, wo_hbm, wg_hbm, wg2_hbm, wu_hbm, wu2_hbm, wd_hbm, wd2_hbm, g_ref, out_ref,
              obuf, wbuf, acc, xr, yall, hbuf, wg, wu, act, rsr, rss,
              o_sem, w_sem, f_sem, d_sem, xs_sem, xr_sem, as_sem, ar_sem, fs_sem, fr_sem, ss_sem, sr_sem):
    me = lax.axis_index('sp')
    chip, core = me // 2, me % 2
    right, left = (chip + 1) % chips, (chip + chips - 1) % chips
    far = (chip + 2) % chips
    ring = (2 * right + core, 2 * left + core)
    peer = 2 * chip + 1 - core
    src = (left, right)
    nt, kt = acc.shape[0], obuf.shape[1] // wbuf.shape[1]
    nbuf, tk, tn = wbuf.shape
    blk = yall.shape[2]
    half = blk // 2
    depth = kt * tk
    shard = wg_hbm.shape[1]

    def slot_of(q):
        return core * (chips - 1) + (1 - 2 * core) * q

    def remote(s, d, ssem, rsem, dev):
        return pltpu.make_async_remote_copy(src_ref=s, dst_ref=d, send_sem=ssem, recv_sem=rsem,
                                            device_id={'sp': dev}, device_id_type=pl.DeviceIdType.MESH)

    def w_copy(t):
        n, k = t // kt, t % kt
        return pltpu.make_async_copy(
            wo_hbm.at[pl.ds(pl.multiple_of(core * depth + k * tk, tk), tk), pl.ds(pl.multiple_of(n * tn, tn), tn)],
            wbuf.at[t % nbuf], w_sem.at[t % nbuf])

    def o_copy(k):
        cols = pl.ds(pl.multiple_of(k * tk, tk), tk)
        return pltpu.make_async_copy(o_hbm.at[:, cols], obuf.at[:, cols], o_sem.at[k])

    f_copies = [pltpu.make_async_copy(s, d.at[:, pl.ds(c * shard, shard)], f_sem.at[i])
                for i, (s, d, c) in enumerate(((wg_hbm, wg, 0), (wg2_hbm, wg, 1), (wu_hbm, wu, 0), (wu2_hbm, wu, 1)))]
    grain = 256
    width = nt * tn
    n_grain = 2 * shard // grain
    per = obuf.shape[0] // grain
    d_copies = []
    for g in range(n_grain):
        s = wd_hbm if g < n_grain // 2 else wd2_hbm
        d_copies.append(pltpu.make_async_copy(
            s.at[pl.ds((g % (n_grain // 2)) * grain, grain), :],
            obuf.at[pl.ds((g % per) * grain, grain), pl.ds((g // per) * width, width)], d_sem.at[g]))

    for k in range(kt):
        o_copy(k).start()
    for t in range(nbuf - 1):
        w_copy(t).start()

    barrier = pltpu.get_barrier_semaphore()
    for dev in (peer,) + ring:
        pl.semaphore_signal(barrier, inc=1, device_id={'sp': dev}, device_id_type=pl.DeviceIdType.MESH)
    pl.semaphore_wait(barrier, 3)

    own_rows = pl.ds(pl.multiple_of(core * blk, blk), blk)
    peer_rows = pl.ds(pl.multiple_of((1 - core) * blk, blk), blk)

    def x_copy(n):
        return remote(acc.at[n, peer_rows, :], xr.at[n], xs_sem.at[n], xr_sem.at[n], peer)

    def a_copy(d, n, slot):
        return remote(yall.at[slot, n], yall.at[slot, n], as_sem.at[d, n], ar_sem.at[d, n], ring[d])

    def f_copy(d, n, slot):
        rows = pl.ds(d * half, half)
        return remote(yall.at[slot, n, rows, :], yall.at[slot, n, rows, :], fs_sem.at[d, n], fr_sem.at[d, n], ring[d])

    def combine(n):
        x_copy(n).wait_recv()
        yall[chip, n] = (acc[n, own_rows, :] + xr[n]).astype(BF16)
        for d in range(2):
            a_copy(d, n, chip).start()

    def forward(n):
        for d in range(2):
            a_copy(d, n, src[d]).wait_recv()
            f_copy(d, n, src[d]).start()

    def w_step(t, _):
        n, k = t // kt, t % kt

        @pl.when(t + nbuf - 1 < nt * kt)
        def _():
            w_copy(t + nbuf - 1).start()

        @pl.when(t == nbuf)
        def _():
            for c in f_copies:
                c.start()

        @pl.when(n == 0)
        def _():
            o_copy(k).wait()
        w_copy(t).wait()
        prod = jnp.dot(obuf[:, pl.ds(pl.multiple_of(k * tk, tk), tk)], wbuf[t % nbuf], preferred_element_type=F32)

        @pl.when(k == 0)
        def _():
            acc[n] = prod

        @pl.when(k > 0)
        def _():
            acc[n] += prod

        @pl.when(k == kt - 1)
        def _():
            x_copy(n).start()

            @pl.when(n >= 1)
            def _():
                combine(n - 1)

            @pl.when(n >= 3)
            def _():
                forward(n - 3)
        return 0

    lax.fori_loop(0, nt * kt, w_step, 0)
    for c in d_copies:
        c.start()
    combine(nt - 1)
    forward(nt - 3)

    def activate(slot):
        def norm(r, _):
            rows = pl.ds(pl.multiple_of(r * 64, 64), 64)
            ys = [yall[slot, k, rows, :].astype(F32) for k in range(nt)]
            total = sum(jnp.sum(y * y, axis=-1, keepdims=True) for y in ys)
            scale = lax.rsqrt(total * (1.0 / width) + 1e-6)
            for k in range(nt):
                gain = g_ref[:, pl.ds(k * tn, tn)].astype(F32)
                hbuf[k, rows, :] = (ys[k] * scale * gain).astype(BF16)
            return 0
        lax.fori_loop(0, blk // 64, norm, 0)

        def cols(c, _):
            cs = pl.ds(pl.multiple_of(c * 256, 256), 256)
            gate = sum(jnp.dot(hbuf[k], wg[pl.ds(k * tn, tn), cs], preferred_element_type=F32) for k in range(nt))
            up = sum(jnp.dot(hbuf[k], wu[pl.ds(k * tn, tn), cs], preferred_element_type=F32) for k in range(nt))
            act[slot, :, cs] = (jax.nn.silu(gate) * up).astype(BF16)
            return 0
        lax.fori_loop(0, 2 * shard // 256, cols, 0)

    hw = width // 2

    def down(slot, c, d):
        rows = pl.ds(c * half, half)
        return sum(jnp.dot(act[slot, rows, pl.ds(g * grain, grain)],
                           obuf[pl.ds((g % per) * grain, grain), pl.ds((g // per) * width + d * hw, hw)],
                           preferred_element_type=F32) for g in range(n_grain))

    def s_copy(d, s, c):
        src_ref = rss.at[d, c] if s == 0 else rsr.at[d, s - 1, c]
        return remote(src_ref, rsr.at[d, s, c], ss_sem.at[d, s, c], sr_sem.at[d, s, c], ring[d])

    def first():
        for d, q in enumerate((left, right)):
            for c in range(2):
                rss[d, c] = down(slot_of(q), c, d)
                s_copy(d, 0, c).start()

    for c in f_copies:
        c.wait()
    activate(chip)
    forward(nt - 2)
    forward(nt - 1)
    for c in d_copies:
        c.wait()
    activate(left)
    activate(right)

    @pl.when(core == 0)
    def _():
        first()
    for n in range(nt):
        for d in range(2):
            f_copy(d, n, far).wait_recv()
    activate(far)

    @pl.when(core == 1)
    def _():
        first()

    for s, dests in ((1, (far, far)), (2, (right, left))):
        for c in range(2):
            for d in range(2):
                part = down(slot_of(dests[d]), c, d)
                s_copy(d, s - 1, c).wait_recv()
                rsr[d, s - 1, c] = rsr[d, s - 1, c] + part
                s_copy(d, s, c).start()

    mine = slot_of(chip)
    per_half = hw // half
    for c in range(2):
        rows = pl.ds(c * half, half)
        for d in range(2):
            part = down(mine, c, d)
            s_copy(d, 2, c).wait_recv()
            pieces = []
            for col in range(d * hw, (d + 1) * hw, 256):
                pieces.append(yall[mine, col // tn, rows, pl.ds(col % tn, 256)].astype(F32))
            y = jnp.concatenate(pieces, axis=1)
            out_ref[rows, pl.ds(d * hw, hw)] = (y + (rsr[d, 2, c] + part)).astype(BF16)

    for n in range(nt):
        x_copy(n).wait_send()
        for d in range(2):
            a_copy(d, n, chip).wait_send()
            f_copy(d, n, src[d]).wait_send()
    for d in range(2):
        for s in range(3):
            for c in range(2):
                s_copy(d, s, c).wait_send()


def tail(chips, o, w_o, w_gate, w_gate2, w_up, w_up2, w_down, w_down2, g_ffn, nbuf=4, tk=1024, tn=512):
    rows, depth = o.shape
    width = w_o.shape[1]
    shard = w_gate.shape[1]
    blk = rows // 2
    nt, kt = width // tn, depth // tk
    dma = pltpu.SemaphoreType.DMA
    hbm = pl.BlockSpec(memory_space=pl.ANY)
    vmem = pl.BlockSpec(memory_space=pltpu.VMEM)
    return pl.pallas_call(
        functools.partial(tail_body, chips),
        in_specs=[hbm] * 8 + [vmem],
        out_specs=vmem,
        out_shape=jax.ShapeDtypeStruct((blk, width), BF16),
        scratch_shapes=[
            pltpu.VMEM((rows, depth), BF16),
            pltpu.VMEM((nbuf, tk, tn), BF16),
            pltpu.VMEM((nt, rows, tn), F32),
            pltpu.VMEM((nt, blk, tn), F32),
            pltpu.VMEM((chips, nt, blk, tn), BF16),
            pltpu.VMEM((nt, blk, tn), BF16),
            pltpu.VMEM((width, 2 * shard), BF16),
            pltpu.VMEM((width, 2 * shard), BF16),
            pltpu.VMEM((chips, blk, 2 * shard), BF16),
            pltpu.VMEM((2, 3, 2, blk // 2, width // 2), F32),
            pltpu.VMEM((2, 2, blk // 2, width // 2), F32),
            dma((kt,)), dma((nbuf,)), dma((4,)), dma((2 * shard // 256,)),
            dma((nt,)), dma((nt,)), dma((2, nt)), dma((2, nt)), dma((2, nt)), dma((2, nt)),
            dma((2, 3, 2)), dma((2, 3, 2)),
        ],
        compiler_params=pltpu.CompilerParams(collective_id=0, has_side_effects=True,
                                             vmem_limit_bytes=63 * 2 ** 20),
        cost_estimate=pl.CostEstimate(flops=46 * 10 ** 9, bytes_accessed=75 * 10 ** 6, transcendentals=10 ** 6),
    )(o, w_o, w_gate, w_gate2, w_up, w_up2, w_down, w_down2, g_ffn)


def solution(mesh):
    group_size = mesh.shape['sp']
    chips = group_size // 2
    tok_spec = P(('dp', 'sp'), None)
    row_spec = P(('dp', 'sp'))
    full_spec = P()
    col_spec = P(None, 'sp')
    swap = [(d, d ^ 1) for d in range(group_size)]

    def device_fn(x_blk, seg_blk, pos_blk, w_dq, g_q, w_uq, w_dkv, g_kv, w_ukv, w_o, g_ffn, w_gate, w_up, w_down):
        me = lax.axis_index('sp')
        chip, core = me // 2, me % 2
        blk_len = x_blk.shape[0]
        core_arr = core.reshape(1).astype(jnp.int32)

        w_gate2 = lax.ppermute(w_gate, 'sp', swap)
        w_up2 = lax.ppermute(w_up, 'sp', swap)
        w_down2 = lax.ppermute(w_down, 'sp', swap)

        cosine, sine = rope_tables(pos_blk)
        tab = jnp.concatenate([cosine, sine, jnp.broadcast_to(pos_blk.astype(F32)[:, None], (blk_len, ROPE_DIM))], axis=1)
        kvr, cqa, cqb, taba, tabb = latents(chips, x_blk, w_dq, g_q, w_dkv, g_kv, tab)

        blk = jnp.stack([2 * chip, group_size - 1 - 2 * chip]).astype(jnp.int32)
        tab = jnp.concatenate([taba, tabb])
        rows_q = (blk[:, None] * blk_len + jnp.arange(blk_len, dtype=jnp.int32)[None, :]).reshape(-1)
        start = rows_q - tab[:, ROPE_DIM].astype(jnp.int32)
        cosine, sine = tab[:, :ROPE_DIM // 2], tab[:, ROPE_DIM // 2:ROPE_DIM]
        cos4 = jnp.concatenate([cosine] * 4, axis=1)
        sin4 = jnp.concatenate([-sine, sine, -sine, sine], axis=1)
        kb = 2 * blk_len
        start = start.reshape(2, 1, blk_len)
        lo = start[:, 0, 0] // kb
        last = (blk * blk_len + blk_len - 1) // kb
        mid = jnp.maximum(jnp.minimum((start[:, 0, -1] + kb - 1) // kb, last), lo)

        o = attention(core_arr, lo, mid, blk, kvr, cqa, cqb, cos4, sin4, start, w_uq, w_ukv, kb)
        return tail(chips, o, w_o, w_gate, w_gate2, w_up, w_up2, w_down, w_down2, g_ffn[None, :])

    return jax.shard_map(device_fn, mesh=mesh, in_specs=(tok_spec, row_spec, row_spec, full_spec, full_spec, full_spec, full_spec, full_spec, full_spec, full_spec, full_spec, col_spec, col_spec, P('sp', None)), out_specs=tok_spec, check_vma=False)
```

```python
import functools
import jax
import jax.numpy as jnp
from jax import lax
from jax.experimental import pallas as pl
from jax.experimental.pallas import tpu as pltpu
from jax.sharding import PartitionSpec as P

NOPE_DIM = 128
ROPE_DIM = 64
VALUE_DIM = 128
KV_LATENT = 512
QK_DIM = NOPE_DIM + ROPE_DIM
KV_DIM = NOPE_DIM + VALUE_DIM
SCORE_SCALE = QK_DIM ** -0.5
LOG2E = 1.4426950408889634
NEG = -2.0e38
F32 = jnp.float32
BF16 = jnp.bfloat16


def rms_norm(vec_in, gain_vec):
    mean_sq = jnp.mean(vec_in * vec_in, axis=-1, keepdims=True)
    return vec_in * lax.rsqrt(mean_sq + 1e-6) * gain_vec.astype(F32)


def rope_tables(positions):
    half_dim = ROPE_DIM // 2
    inv_freq = 10000.0 ** (-jnp.arange(half_dim, dtype=F32) / half_dim)
    angles = positions.astype(F32)[..., None] * inv_freq
    return jnp.cos(angles), jnp.sin(angles)


def latent_body(chips, x_hbm, wdq_hbm, gq_ref, wdkv_hbm, gkv_ref, tab_ref,
                kvr_ref, cqa_ref, cqb_ref, taba_ref, tabb_ref, cq_s, x_ref, wdq_ref, wdkv_ref,
                in_sem, rs_sem, rr_sem, fs_sem, fr_sem, ps_sem, pr_sem, qs_sem, qr_sem):
    me = lax.axis_index('sp')
    chip, core = me // 2, me % 2
    right, left = (chip + 1) % chips, (chip + chips - 1) % chips
    far = (chip + 2) % chips
    ring = (2 * right + core, 2 * left + core)
    src = (left, right)
    peer = 2 * chip + 1 - core
    mirror = chips - 1 - chip
    blk = x_ref.shape[0]
    half = blk // 2
    loads = [pltpu.make_async_copy(s, d, in_sem.at[i])
             for i, (s, d) in enumerate(((x_hbm, x_ref), (wdkv_hbm, wdkv_ref), (wdq_hbm, wdq_ref)))]
    for c in loads:
        c.start()

    def remote(s, d, ssem, rsem, dev):
        return pltpu.make_async_remote_copy(src_ref=s, dst_ref=d, send_sem=ssem, recv_sem=rsem,
                                            device_id={'sp': dev}, device_id_type=pl.DeviceIdType.MESH)

    barrier = pltpu.get_barrier_semaphore()
    for dev in (peer,) + ring + (2 * mirror + 1 - core,):
        pl.semaphore_signal(barrier, inc=1, device_id={'sp': dev}, device_id_type=pl.DeviceIdType.MESH)

    def block(c, k, part=None):
        start = (2 * c + k) * blk
        if part is None:
            return kvr_ref.at[pl.ds(pl.multiple_of(start, blk), blk), :]
        return kvr_ref.at[pl.ds(pl.multiple_of(start + part * half, half), half), :]

    def ring_copy(d, c):
        return remote(block(c, core), block(c, core), rs_sem.at[d], rr_sem.at[d], ring[d])

    def fwd_copy(d, c):
        return remote(block(c, core, d), block(c, core, d), fs_sem.at[d], fr_sem.at[d], ring[d])

    def peer_copy(i, c, k, part=None):
        return remote(block(c, k, part), block(c, k, part), ps_sem.at[i], pr_sem.at[i], peer)

    loads[0].wait()
    loads[1].wait()
    x = x_ref[...]
    lat = wdkv_ref.shape[0] - ROPE_DIM
    nt_dims = (((1,), (1,)), ((), ()))
    kv = lax.dot_general(x, wdkv_ref[:lat, :], nt_dims, preferred_element_type=F32)
    c_kv = rms_norm(kv, gkv_ref[...]).astype(BF16)
    kr = lax.dot_general(x, wdkv_ref[lat:, :], nt_dims, preferred_element_type=F32)
    hd = ROPE_DIM // 2
    cosine, sine = tab_ref[:, :hd], tab_ref[:, hd:2 * hd]
    lo_half, hi_half = kr[:, :hd], kr[:, hd:]
    kr = jnp.concatenate([lo_half * cosine - hi_half * sine, hi_half * cosine + lo_half * sine,
                          jnp.zeros((blk, ROPE_DIM), F32)], axis=1)
    own = pl.ds(pl.multiple_of(me * blk, blk), blk)
    kvr_ref[own, :lat] = c_kv
    kvr_ref[own, lat:] = kr.astype(BF16)

    pl.semaphore_wait(barrier, 4)
    for d in range(2):
        ring_copy(d, chip).start()
    peer_copy(0, chip, core).start()

    loads[2].wait()
    cq_s[...] = rms_norm(jnp.dot(x, wdq_ref[...], preferred_element_type=F32), gq_ref[...]).astype(BF16)
    pairs = ((0, cq_s, cqa_ref, cqb_ref), (1, tab_ref, taba_ref, tabb_ref))

    def qa_copy(i, s, a):
        return remote(s, a, qs_sem.at[i], qr_sem.at[i], peer)

    def qb_copy(i, s, b, k):
        return remote(s, b, qs_sem.at[2 * k + i], qr_sem.at[2 + i], 2 * mirror + k)

    @pl.when(core == 0)
    def _():
        for i, s, a, b in pairs:
            qa_copy(i, s, a).start()
        cqa_ref[...] = cq_s[...]
        taba_ref[...] = tab_ref[...]

    @pl.when(core == 1)
    def _():
        for i, s, a, b in pairs:
            for k in range(2):
                qb_copy(i, s, b, k).start()

    for d in range(2):
        ring_copy(d, src[d]).wait_recv()
        fwd_copy(d, src[d]).start()
        peer_copy(1 + d, src[d], core).start()
    for d in range(2):
        fwd_copy(d, far).wait_recv()
        peer_copy(3 + d, far, core, d).start()

    for i, s, a, b in pairs:
        qb_copy(i, s, b, 0).wait_recv()

    @pl.when(core == 1)
    def _():
        for i, s, a, b in pairs:
            qa_copy(i, s, a).wait_recv()
            for k in range(2):
                qb_copy(i, s, b, k).wait_send()

    @pl.when(core == 0)
    def _():
        for i, s, a, b in pairs:
            qa_copy(i, s, a).wait_send()

    other = 1 - core
    waits = ((0, chip, None), (1, left, None), (2, right, None), (3, far, 0), (4, far, 1))
    for i, c, part in waits:
        peer_copy(i, c, other, part).wait_recv()
    for i, c, part in waits:
        peer_copy(i, c, core, part).wait_send()
    for d in range(2):
        ring_copy(d, chip).wait_send()
        fwd_copy(d, src[d]).wait_send()


def latents(chips, x, w_dq, g_q, w_dkv, g_kv, tab):
    blk = x.shape[0]
    lat = w_dkv.shape[0] - ROPE_DIM
    tok = 2 * chips * blk
    dma = pltpu.SemaphoreType.DMA
    hbm = pl.BlockSpec(memory_space=pl.ANY)
    vmem = pl.BlockSpec(memory_space=pltpu.VMEM)
    shape = jax.ShapeDtypeStruct
    return pl.pallas_call(
        functools.partial(latent_body, chips),
        in_specs=[hbm, hbm, vmem, hbm, vmem, vmem],
        out_specs=[vmem] * 5,
        out_shape=[shape((tok, lat + 2 * ROPE_DIM), BF16), shape((blk, w_dq.shape[1]), BF16),
                   shape((blk, w_dq.shape[1]), BF16), shape(tab.shape, F32), shape(tab.shape, F32)],
        scratch_shapes=[pltpu.VMEM((blk, w_dq.shape[1]), BF16), pltpu.VMEM(x.shape, BF16),
                        pltpu.VMEM(w_dq.shape, BF16), pltpu.VMEM(w_dkv.shape, BF16), dma((3,))] + [dma((2,))] * 4 + [dma((5,))] * 2 + [dma((4,))] * 2,
        compiler_params=pltpu.CompilerParams(collective_id=1, has_side_effects=True, vmem_limit_bytes=62 * 2 ** 20),
        cost_estimate=pl.CostEstimate(flops=2 * 10 ** 9, bytes_accessed=10 ** 7, transcendentals=0),
    )(x, w_dq, g_q[None, :], w_dkv, g_kv[None, :], tab)


def attn_body(core_ref, lo_ref, mid_ref, blk_ref, kvr_ref, cqa_ref, cqb_ref, cos_ref, sin_ref, start_ref,
              wuq_ref, wukv_ref, o_ref, kcat, vt, qcat, sbuf, mbuf, acc, *, kb):
    i = pl.program_id(0)
    tok = kvr_ref.shape[0]
    qb = cqa_ref.shape[0]
    cur, prev = i % 2, (i + 1) % 2
    v_new, v_old = i % 3, (i + 1) % 3
    n_piece = tok // kb

    @pl.when(i == 0)
    def _():
        for par in range(2):
            for h in range(2):
                kcat[par, h, :, NOPE_DIM:] = kvr_ref[:, KV_LATENT:]

    def kv_piece(pc):
        rows = pl.ds(pl.multiple_of(pc * kb, kb), kb)
        e = jnp.dot(kvr_ref[rows, :KV_LATENT], wukv_ref[...], preferred_element_type=F32).astype(BF16)
        for h in range(2):
            kcat[cur, h, rows, :NOPE_DIM] = e[:, KV_DIM * h:KV_DIM * h + NOPE_DIM]
            vt[v_new, h, :, rows] = e[:, KV_DIM * h + NOPE_DIM:KV_DIM * (h + 1)].T

    def q_piece():
        for b, cq in enumerate((cqa_ref, cqb_ref)):
            rows = pl.ds(b * qb, qb)
            q = jnp.dot(cq[...], wuq_ref[...], preferred_element_type=F32)
            q_r = jnp.concatenate([q[:, NOPE_DIM:QK_DIM], q[:, QK_DIM + NOPE_DIM:]], axis=1)
            lane = lax.broadcasted_iota(jnp.int32, q_r.shape, 1)
            lo_half = (lane % ROPE_DIM) < (ROPE_DIM // 2)
            swapped = jnp.where(lo_half, pltpu.roll(q_r, 2 * ROPE_DIM - ROPE_DIM // 2, 1),
                                pltpu.roll(q_r, ROPE_DIM // 2, 1))
            q_r = (q_r * cos_ref[rows, :] + swapped * sin_ref[rows, :]).astype(BF16)
            zero = jnp.zeros((qb, ROPE_DIM), BF16)
            for h in range(2):
                qcat[cur, b, h, :, :NOPE_DIM] = q[:, QK_DIM * h:QK_DIM * h + NOPE_DIM].astype(BF16)
                qcat[cur, b, h, :, NOPE_DIM:] = jnp.concatenate([q_r[:, ROPE_DIM * h:ROPE_DIM * (h + 1)], zero], axis=1)

    @pl.when(i == 0)
    def _():
        q_piece()
        lax.fori_loop(0, n_piece, lambda pc, c: (kv_piece(pc), c)[1], 0)

    @pl.when(i > 0)
    def _():
        base = 0
        for b in range(2):
            t0 = blk_ref[b] * qb
            lo = lo_ref[b]
            last = (t0 + qb - 1) // kb

            def step(j, carry, masked, piece, b=b, t0=t0):
                k0 = pl.multiple_of(j * kb, kb)
                krows = pl.ds(k0, kb)
                new = []
                for h in range(2):
                    m, l = carry[2 * h], carry[2 * h + 1]
                    p = jnp.exp2(sbuf[b, h, krows, :] - mbuf[b, h])
                    s = lax.dot_general(kcat[prev, h, krows, :], qcat[prev, b, h], (((1,), (1,)), ((), ())),
                                        preferred_element_type=F32)
                    s = s * (SCORE_SCALE * LOG2E)
                    if masked:
                        r = k0 + lax.broadcasted_iota(jnp.int32, s.shape, 0)
                        t = t0 + lax.broadcasted_iota(jnp.int32, s.shape, 1)
                        s = jnp.where((r <= t) & (r >= start_ref[b]), s, NEG)
                    m = jnp.maximum(m, jnp.max(s.reshape(kb // 8, 8, qb), axis=0))
                    l = l + jnp.sum(p.reshape(kb // 8, 8, qb), axis=0)
                    acc[h] += jnp.dot(vt[v_old, h, :, krows], p.astype(BF16), preferred_element_type=F32)
                    sbuf[b, h, krows, :] = s
                    new += [m, l]
                piece(j)
                return tuple(new)

            piece = lambda j, off=base - lo: kv_piece(off + j)
            acc[...] = jnp.zeros_like(acc)
            carry = (jnp.full((8, qb), NEG, F32), jnp.zeros((8, qb), F32)) * 2
            carry = lax.fori_loop(lo, mid_ref[b], functools.partial(step, masked=True, piece=piece), carry)
            carry = lax.fori_loop(mid_ref[b], last, functools.partial(step, masked=False, piece=piece), carry)
            carry = step(last, carry, True, piece if b == 0 else lambda j: q_piece())
            base = base + (last - lo + 1 if b == 0 else last - lo)
            for h in range(2):
                mbuf[b, h] = jnp.max(carry[2 * h], axis=0, keepdims=True)
                l = jnp.sum(carry[2 * h + 1], axis=0, keepdims=True)
                o = (acc[h] * (1.0 / l)).astype(BF16)
                o_ref[pl.ds(b * qb, qb), VALUE_DIM * h:VALUE_DIM * (h + 1)] = o.T
        lax.fori_loop(base, n_piece, lambda pc, c: (kv_piece(pc), c)[1], 0)


def attention(core, lo, mid, blk, kvr, cqa, cqb, cos, sin, start, w_uq, w_ukv, kb):
    tok = kvr.shape[0]
    qb, q_lat = cqa.shape
    heads = w_uq.shape[1] // QK_DIM
    pairs = heads // 4
    full = lambda shape: pl.BlockSpec(shape, lambda i, *_: (0,) * len(shape), pipeline_mode=pl.Buffered(1))
    group = lambda i, core: core[0] * pairs + jnp.minimum(i, pairs - 1)
    return pl.pallas_call(
        functools.partial(attn_body, kb=kb),
        grid_spec=pltpu.PrefetchScalarGridSpec(
            num_scalar_prefetch=4,
            grid=(pairs + 2,),
            in_specs=[
                full(kvr.shape), full(cqa.shape), full(cqb.shape), full(cos.shape), full(sin.shape), full(start.shape),
                pl.BlockSpec((q_lat, 2 * QK_DIM), lambda i, core, *_: (0, group(i, core))),
                pl.BlockSpec((KV_LATENT, 2 * KV_DIM), lambda i, core, *_: (0, group(i, core))),
            ],
            out_specs=pl.BlockSpec((2 * qb, 2 * VALUE_DIM), lambda i, *_: (0, jnp.maximum(i - 2, 0))),
            scratch_shapes=[
                pltpu.VMEM((2, 2, tok, 2 * NOPE_DIM), BF16),
                pltpu.VMEM((3, 2, VALUE_DIM, tok), BF16),
                pltpu.VMEM((2, 2, 2, qb, 2 * NOPE_DIM), BF16),
                pltpu.VMEM((2, 2, tok, qb), F32),
                pltpu.VMEM((2, 2, 1, qb), F32),
                pltpu.VMEM((2, VALUE_DIM, qb), F32),
            ]),
        out_shape=jax.ShapeDtypeStruct((2 * qb, heads // 2 * VALUE_DIM), BF16),
        compiler_params=pltpu.CompilerParams(dimension_semantics=("arbitrary",), vmem_limit_bytes=62 * 2 ** 20),
        cost_estimate=pl.CostEstimate(flops=80 * 10 ** 9, bytes_accessed=45 * 10 ** 6, transcendentals=40 * 10 ** 6),
    )(core, lo, mid, blk, kvr, cqa, cqb, cos, sin, start, w_uq, w_ukv)


def tail_body(chips, o_hbm, wo_hbm, wg_hbm, wg2_hbm, wu_hbm, wu2_hbm, wd_hbm, wd2_hbm, g_ref, out_ref,
              obuf, wbuf, acc, xr, yall, hbuf, wg, wu, act, rsr, rss,
              o_sem, w_sem, f_sem, d_sem, xs_sem, xr_sem, as_sem, ar_sem, fs_sem, fr_sem, ss_sem, sr_sem):
    me = lax.axis_index('sp')
    chip, core = me // 2, me % 2
    right, left = (chip + 1) % chips, (chip + chips - 1) % chips
    far = (chip + 2) % chips
    ring = (2 * right + core, 2 * left + core)
    peer = 2 * chip + 1 - core
    src = (left, right)
    nt, kt = acc.shape[0], obuf.shape[1] // wbuf.shape[1]
    nbuf, tk, tn = wbuf.shape
    blk = yall.shape[2]
    half = blk // 2
    depth = kt * tk
    shard = wg_hbm.shape[1]

    def slot_of(q):
        return core * (chips - 1) + (1 - 2 * core) * q

    def remote(s, d, ssem, rsem, dev):
        return pltpu.make_async_remote_copy(src_ref=s, dst_ref=d, send_sem=ssem, recv_sem=rsem,
                                            device_id={'sp': dev}, device_id_type=pl.DeviceIdType.MESH)

    def w_copy(t):
        n, k = t // kt, t % kt
        return pltpu.make_async_copy(
            wo_hbm.at[pl.ds(pl.multiple_of(core * depth + k * tk, tk), tk), pl.ds(pl.multiple_of(n * tn, tn), tn)],
            wbuf.at[t % nbuf], w_sem.at[t % nbuf])

    def o_copy(k):
        cols = pl.ds(pl.multiple_of(k * tk, tk), tk)
        return pltpu.make_async_copy(o_hbm.at[:, cols], obuf.at[:, cols], o_sem.at[k])

    f_copies = [pltpu.make_async_copy(s, d.at[:, pl.ds(c * shard, shard)], f_sem.at[i])
                for i, (s, d, c) in enumerate(((wg_hbm, wg, 0), (wg2_hbm, wg, 1), (wu_hbm, wu, 0), (wu2_hbm, wu, 1)))]
    grain = 256
    width = nt * tn
    n_grain = 2 * shard // grain
    per = obuf.shape[0] // grain
    d_copies = []
    for g in range(n_grain):
        s = wd_hbm if g < n_grain // 2 else wd2_hbm
        d_copies.append(pltpu.make_async_copy(
            s.at[pl.ds((g % (n_grain // 2)) * grain, grain), :],
            obuf.at[pl.ds((g % per) * grain, grain), pl.ds((g // per) * width, width)], d_sem.at[g]))

    for k in range(kt):
        o_copy(k).start()
    for t in range(nbuf - 1):
        w_copy(t).start()

    barrier = pltpu.get_barrier_semaphore()
    for dev in (peer,) + ring:
        pl.semaphore_signal(barrier, inc=1, device_id={'sp': dev}, device_id_type=pl.DeviceIdType.MESH)
    pl.semaphore_wait(barrier, 3)

    own_rows = pl.ds(pl.multiple_of(core * blk, blk), blk)
    peer_rows = pl.ds(pl.multiple_of((1 - core) * blk, blk), blk)

    def x_copy(n):
        return remote(acc.at[n, peer_rows, :], xr.at[n], xs_sem.at[n], xr_sem.at[n], peer)

    def a_copy(d, n, slot):
        return remote(yall.at[slot, n], yall.at[slot, n], as_sem.at[d, n], ar_sem.at[d, n], ring[d])

    def f_copy(d, n, slot):
        rows = pl.ds(d * half, half)
        return remote(yall.at[slot, n, rows, :], yall.at[slot, n, rows, :], fs_sem.at[d, n], fr_sem.at[d, n], ring[d])

    def combine(n):
        x_copy(n).wait_recv()
        yall[chip, n] = (acc[n, own_rows, :] + xr[n]).astype(BF16)
        for d in range(2):
            a_copy(d, n, chip).start()

    def forward(n):
        for d in range(2):
            a_copy(d, n, src[d]).wait_recv()
            f_copy(d, n, src[d]).start()

    def w_step(t, _):
        n, k = t // kt, t % kt

        @pl.when(t + nbuf - 1 < nt * kt)
        def _():
            w_copy(t + nbuf - 1).start()

        @pl.when(t == nbuf)
        def _():
            for c in f_copies:
                c.start()

        @pl.when(n == 0)
        def _():
            o_copy(k).wait()
        w_copy(t).wait()
        prod = jnp.dot(obuf[:, pl.ds(pl.multiple_of(k * tk, tk), tk)], wbuf[t % nbuf], preferred_element_type=F32)

        @pl.when(k == 0)
        def _():
            acc[n] = prod

        @pl.when(k > 0)
        def _():
            acc[n] += prod

        @pl.when(k == kt - 1)
        def _():
            x_copy(n).start()

            @pl.when(n >= 1)
            def _():
                combine(n - 1)

            @pl.when(n >= 3)
            def _():
                forward(n - 3)
        return 0

    lax.fori_loop(0, nt * kt, w_step, 0)
    for c in d_copies:
        c.start()
    combine(nt - 1)
    forward(nt - 3)

    def activate(slot):
        def norm(r, _):
            rows = pl.ds(pl.multiple_of(r * 64, 64), 64)
            ys = [yall[slot, k, rows, :].astype(F32) for k in range(nt)]
            total = sum(jnp.sum(y * y, axis=-1, keepdims=True) for y in ys)
            scale = lax.rsqrt(total * (1.0 / width) + 1e-6)
            for k in range(nt):
                gain = g_ref[:, pl.ds(k * tn, tn)].astype(F32)
                hbuf[k, rows, :] = (ys[k] * scale * gain).astype(BF16)
            return 0
        lax.fori_loop(0, blk // 64, norm, 0)

        def cols(c, _):
            cs = pl.ds(pl.multiple_of(c * 256, 256), 256)
            gate = sum(jnp.dot(hbuf[k], wg[pl.ds(k * tn, tn), cs], preferred_element_type=F32) for k in range(nt))
            up = sum(jnp.dot(hbuf[k], wu[pl.ds(k * tn, tn), cs], preferred_element_type=F32) for k in range(nt))
            act[slot, :, cs] = (jax.nn.silu(gate) * up).astype(BF16)
            return 0
        lax.fori_loop(0, 2 * shard // 256, cols, 0)

    hw = width // 2

    def down(slot, c, d):
        rows = pl.ds(c * half, half)
        return sum(jnp.dot(act[slot, rows, pl.ds(g * grain, grain)],
                           obuf[pl.ds((g % per) * grain, grain), pl.ds((g // per) * width + d * hw, hw)],
                           preferred_element_type=F32) for g in range(n_grain))

    def s_copy(d, s, c):
        src_ref = rss.at[d, c] if s == 0 else rsr.at[d, s - 1, c]
        return remote(src_ref, rsr.at[d, s, c], ss_sem.at[d, s, c], sr_sem.at[d, s, c], ring[d])

    def first():
        for d, q in enumerate((left, right)):
            for c in range(2):
                rss[d, c] = down(slot_of(q), c, d)
                s_copy(d, 0, c).start()

    for c in f_copies:
        c.wait()
    activate(chip)
    forward(nt - 2)
    forward(nt - 1)
    for c in d_copies:
        c.wait()
    activate(left)
    activate(right)

    @pl.when(core == 0)
    def _():
        first()
    for n in range(nt):
        for d in range(2):
            f_copy(d, n, far).wait_recv()
    activate(far)

    @pl.when(core == 1)
    def _():
        first()

    for s, dests in ((1, (far, far)), (2, (right, left))):
        for c in range(2):
            for d in range(2):
                part = down(slot_of(dests[d]), c, d)
                s_copy(d, s - 1, c).wait_recv()
                rsr[d, s - 1, c] = rsr[d, s - 1, c] + part
                s_copy(d, s, c).start()

    mine = slot_of(chip)
    per_half = hw // half
    for c in range(2):
        rows = pl.ds(c * half, half)
        for d in range(2):
            part = down(mine, c, d)
            s_copy(d, 2, c).wait_recv()
            pieces = []
            for col in range(d * hw, (d + 1) * hw, 256):
                pieces.append(yall[mine, col // tn, rows, pl.ds(col % tn, 256)].astype(F32))
            y = jnp.concatenate(pieces, axis=1)
            out_ref[rows, pl.ds(d * hw, hw)] = (y + (rsr[d, 2, c] + part)).astype(BF16)

    for n in range(nt):
        x_copy(n).wait_send()
        for d in range(2):
            a_copy(d, n, chip).wait_send()
            f_copy(d, n, src[d]).wait_send()
    for d in range(2):
        for s in range(3):
            for c in range(2):
                s_copy(d, s, c).wait_send()


def tail(chips, o, w_o, w_gate, w_gate2, w_up, w_up2, w_down, w_down2, g_ffn, nbuf=4, tk=1024, tn=512):
    rows, depth = o.shape
    width = w_o.shape[1]
    shard = w_gate.shape[1]
    blk = rows // 2
    nt, kt = width // tn, depth // tk
    dma = pltpu.SemaphoreType.DMA
    hbm = pl.BlockSpec(memory_space=pl.ANY)
    vmem = pl.BlockSpec(memory_space=pltpu.VMEM)
    return pl.pallas_call(
        functools.partial(tail_body, chips),
        in_specs=[hbm] * 8 + [vmem],
        out_specs=vmem,
        out_shape=jax.ShapeDtypeStruct((blk, width), BF16),
        scratch_shapes=[
            pltpu.VMEM((rows, depth), BF16),
            pltpu.VMEM((nbuf, tk, tn), BF16),
            pltpu.VMEM((nt, rows, tn), F32),
            pltpu.VMEM((nt, blk, tn), F32),
            pltpu.VMEM((chips, nt, blk, tn), BF16),
            pltpu.VMEM((nt, blk, tn), BF16),
            pltpu.VMEM((width, 2 * shard), BF16),
            pltpu.VMEM((width, 2 * shard), BF16),
            pltpu.VMEM((chips, blk, 2 * shard), BF16),
            pltpu.VMEM((2, 3, 2, blk // 2, width // 2), F32),
            pltpu.VMEM((2, 2, blk // 2, width // 2), F32),
            dma((kt,)), dma((nbuf,)), dma((4,)), dma((2 * shard // 256,)),
            dma((nt,)), dma((nt,)), dma((2, nt)), dma((2, nt)), dma((2, nt)), dma((2, nt)),
            dma((2, 3, 2)), dma((2, 3, 2)),
        ],
        compiler_params=pltpu.CompilerParams(collective_id=0, has_side_effects=True,
                                             vmem_limit_bytes=63 * 2 ** 20),
        cost_estimate=pl.CostEstimate(flops=46 * 10 ** 9, bytes_accessed=75 * 10 ** 6, transcendentals=10 ** 6),
    )(o, w_o, w_gate, w_gate2, w_up, w_up2, w_down, w_down2, g_ffn)


def solution(mesh):
    group_size = mesh.shape['sp']
    chips = group_size // 2
    tok_spec = P(('dp', 'sp'), None)
    row_spec = P(('dp', 'sp'))
    full_spec = P()
    col_spec = P(None, 'sp')
    swap = [(d, d ^ 1) for d in range(group_size)]

    def device_fn(x_blk, seg_blk, pos_blk, w_dq, g_q, w_uq, w_dkv, g_kv, w_ukv, w_o, g_ffn, w_gate, w_up, w_down):
        me = lax.axis_index('sp')
        chip, core = me // 2, me % 2
        blk_len = x_blk.shape[0]
        core_arr = core.reshape(1).astype(jnp.int32)

        cosine, sine = rope_tables(pos_blk)
        tab = jnp.concatenate([cosine, sine, jnp.broadcast_to(pos_blk.astype(F32)[:, None], (blk_len, ROPE_DIM))], axis=1)
        kvr, cqa, cqb, taba, tabb = latents(chips, x_blk, w_dq, g_q, w_dkv.T, g_kv, tab)
        kvr, late_gate, late_up, late_down = lax.optimization_barrier((kvr, w_gate, w_up, w_down))
        w_gate2 = lax.ppermute(late_gate, 'sp', swap)
        w_up2 = lax.ppermute(late_up, 'sp', swap)
        w_down2 = lax.ppermute(late_down, 'sp', swap)

        blk = jnp.stack([2 * chip, group_size - 1 - 2 * chip]).astype(jnp.int32)
        tab = jnp.concatenate([taba, tabb])
        rows_q = (blk[:, None] * blk_len + jnp.arange(blk_len, dtype=jnp.int32)[None, :]).reshape(-1)
        start = rows_q - tab[:, ROPE_DIM].astype(jnp.int32)
        cosine, sine = tab[:, :ROPE_DIM // 2], tab[:, ROPE_DIM // 2:ROPE_DIM]
        cos4 = jnp.concatenate([cosine] * 4, axis=1)
        sin4 = jnp.concatenate([-sine, sine, -sine, sine], axis=1)
        kb = 2 * blk_len
        start = start.reshape(2, 1, blk_len)
        lo = start[:, 0, 0] // kb
        last = (blk * blk_len + blk_len - 1) // kb
        mid = jnp.maximum(jnp.minimum((start[:, 0, -1] + kb - 1) // kb, last), lo)

        o = attention(core_arr, lo, mid, blk, kvr, cqa, cqb, cos4, sin4, start, w_uq, w_ukv, kb)
        return tail(chips, o, w_o, w_gate, w_gate2, w_up, w_up2, w_down, w_down2, g_ffn[None, :])

    return jax.shard_map(device_fn, mesh=mesh, in_specs=(tok_spec, row_spec, row_spec, full_spec, full_spec, full_spec, full_spec, full_spec, full_spec, full_spec, full_spec, col_spec, col_spec, P('sp', None)), out_specs=tok_spec, check_vma=False)
```

```python
import functools
import jax
import jax.numpy as jnp
from jax import lax
from jax.experimental import pallas as pl
from jax.experimental.pallas import tpu as pltpu
from jax.sharding import PartitionSpec as P

NOPE_DIM = 128
ROPE_DIM = 64
VALUE_DIM = 128
KV_LATENT = 512
QK_DIM = NOPE_DIM + ROPE_DIM
KV_DIM = NOPE_DIM + VALUE_DIM
SCORE_SCALE = QK_DIM ** -0.5
LOG2E = 1.4426950408889634
NEG = -2.0e38
F32 = jnp.float32
BF16 = jnp.bfloat16


def rms_norm(vec_in, gain_vec):
    mean_sq = jnp.mean(vec_in * vec_in, axis=-1, keepdims=True)
    return vec_in * lax.rsqrt(mean_sq + 1e-6) * gain_vec.astype(F32)


def rope_tables(positions):
    half_dim = ROPE_DIM // 2
    inv_freq = 10000.0 ** (-jnp.arange(half_dim, dtype=F32) / half_dim)
    angles = positions.astype(F32)[..., None] * inv_freq
    return jnp.cos(angles), jnp.sin(angles)


def latent_body(chips, x_hbm, wdq_hbm, gq_ref, wdkv_hbm, gkv_ref, tab_ref,
                kvr_ref, cqa_ref, cqb_ref, taba_ref, tabb_ref, cq_s, x_ref, wdq_ref, wdkv_ref,
                in_sem, rs_sem, rr_sem, fs_sem, fr_sem, ps_sem, pr_sem, qs_sem, qr_sem):
    me = lax.axis_index('sp')
    chip, core = me // 2, me % 2
    right, left = (chip + 1) % chips, (chip + chips - 1) % chips
    far = (chip + 2) % chips
    ring = (2 * right + core, 2 * left + core)
    src = (left, right)
    peer = 2 * chip + 1 - core
    mirror = chips - 1 - chip
    blk = x_ref.shape[0]
    half = blk // 2
    loads = [pltpu.make_async_copy(s, d, in_sem.at[i])
             for i, (s, d) in enumerate(((x_hbm, x_ref), (wdkv_hbm, wdkv_ref), (wdq_hbm, wdq_ref)))]
    for c in loads:
        c.start()

    def remote(s, d, ssem, rsem, dev):
        return pltpu.make_async_remote_copy(src_ref=s, dst_ref=d, send_sem=ssem, recv_sem=rsem,
                                            device_id={'sp': dev}, device_id_type=pl.DeviceIdType.MESH)

    barrier = pltpu.get_barrier_semaphore()
    for dev in (peer,) + ring:
        pl.semaphore_signal(barrier, inc=1, device_id={'sp': dev}, device_id_type=pl.DeviceIdType.MESH)

    def block(c, k, part=None):
        start = (2 * c + k) * blk
        if part is None:
            return kvr_ref.at[pl.ds(pl.multiple_of(start, blk), blk), :]
        return kvr_ref.at[pl.ds(pl.multiple_of(start + part * half, half), half), :]

    def ring_copy(d, c):
        return remote(block(c, core), block(c, core), rs_sem.at[d], rr_sem.at[d], ring[d])

    def fwd_copy(d, c):
        return remote(block(c, core, d), block(c, core, d), fs_sem.at[d], fr_sem.at[d], ring[d])

    def peer_copy(i, c, k, part=None):
        return remote(block(c, k, part), block(c, k, part), ps_sem.at[i], pr_sem.at[i], peer)

    loads[0].wait()
    loads[1].wait()
    x = x_ref[...]
    lat = wdkv_ref.shape[0] - ROPE_DIM
    nt_dims = (((1,), (1,)), ((), ()))
    kv = lax.dot_general(x, wdkv_ref[:lat, :], nt_dims, preferred_element_type=F32)
    c_kv = rms_norm(kv, gkv_ref[...]).astype(BF16)
    kr = lax.dot_general(x, wdkv_ref[lat:, :], nt_dims, preferred_element_type=F32)
    hd = ROPE_DIM // 2
    cosine, sine = tab_ref[:, :hd], tab_ref[:, hd:2 * hd]
    lo_half, hi_half = kr[:, :hd], kr[:, hd:]
    kr = jnp.concatenate([lo_half * cosine - hi_half * sine, hi_half * cosine + lo_half * sine,
                          jnp.zeros((blk, ROPE_DIM), F32)], axis=1)
    own = pl.ds(pl.multiple_of(me * blk, blk), blk)
    kvr_ref[own, :lat] = c_kv
    kvr_ref[own, lat:] = kr.astype(BF16)

    pl.semaphore_wait(barrier, 3)
    for d in range(2):
        ring_copy(d, chip).start()
    peer_copy(0, chip, core).start()

    loads[2].wait()
    cq_s[...] = rms_norm(jnp.dot(x, wdq_ref[...], preferred_element_type=F32), gq_ref[...]).astype(BF16)
    pairs = ((0, cq_s, cqa_ref, cqb_ref), (1, tab_ref, taba_ref, tabb_ref))

    def qa_copy(i, s, a):
        return remote(s, a, qs_sem.at[i], qr_sem.at[i], peer)

    def qb_copy(i, s, b):
        return remote(s, b, qs_sem.at[i], qr_sem.at[2 + i], 2 * mirror + core)

    def qc_copy(i, b):
        return remote(b, b, qs_sem.at[2 + i], qr_sem.at[2 + i], peer)

    @pl.when(core == 0)
    def _():
        for i, s, a, b in pairs:
            qa_copy(i, s, a).start()
        cqa_ref[...] = cq_s[...]
        taba_ref[...] = tab_ref[...]

    @pl.when(core == 1)
    def _():
        for i, s, a, b in pairs:
            qb_copy(i, s, b).start()

    for d in range(2):
        ring_copy(d, src[d]).wait_recv()
        fwd_copy(d, src[d]).start()
        peer_copy(1 + d, src[d], core).start()
    for d in range(2):
        fwd_copy(d, far).wait_recv()
        peer_copy(3 + d, far, core, d).start()

    @pl.when(core == 1)
    def _():
        for i, s, a, b in pairs:
            qb_copy(i, s, b).wait_recv()
            qc_copy(i, b).start()
        for i, s, a, b in pairs:
            qa_copy(i, s, a).wait_recv()
            qb_copy(i, s, b).wait_send()
            qc_copy(i, b).wait_send()

    @pl.when(core == 0)
    def _():
        for i, s, a, b in pairs:
            qc_copy(i, b).wait_recv()
            qa_copy(i, s, a).wait_send()

    other = 1 - core
    waits = ((0, chip, None), (1, left, None), (2, right, None), (3, far, 0), (4, far, 1))
    for i, c, part in waits:
        peer_copy(i, c, other, part).wait_recv()
    for i, c, part in waits:
        peer_copy(i, c, core, part).wait_send()
    for d in range(2):
        ring_copy(d, chip).wait_send()
        fwd_copy(d, src[d]).wait_send()


def latents(chips, x, w_dq, g_q, w_dkv, g_kv, tab):
    blk = x.shape[0]
    lat = w_dkv.shape[0] - ROPE_DIM
    tok = 2 * chips * blk
    dma = pltpu.SemaphoreType.DMA
    hbm = pl.BlockSpec(memory_space=pl.ANY)
    vmem = pl.BlockSpec(memory_space=pltpu.VMEM)
    shape = jax.ShapeDtypeStruct
    return pl.pallas_call(
        functools.partial(latent_body, chips),
        in_specs=[hbm, hbm, vmem, hbm, vmem, vmem],
        out_specs=[vmem] * 5,
        out_shape=[shape((tok, lat + 2 * ROPE_DIM), BF16), shape((blk, w_dq.shape[1]), BF16),
                   shape((blk, w_dq.shape[1]), BF16), shape(tab.shape, F32), shape(tab.shape, F32)],
        scratch_shapes=[pltpu.VMEM((blk, w_dq.shape[1]), BF16), pltpu.VMEM(x.shape, BF16),
                        pltpu.VMEM(w_dq.shape, BF16), pltpu.VMEM(w_dkv.shape, BF16), dma((3,))] + [dma((2,))] * 4 + [dma((5,))] * 2 + [dma((4,))] * 2,
        compiler_params=pltpu.CompilerParams(collective_id=1, has_side_effects=True, vmem_limit_bytes=62 * 2 ** 20),
        cost_estimate=pl.CostEstimate(flops=2 * 10 ** 9, bytes_accessed=10 ** 7, transcendentals=0),
    )(x, w_dq, g_q[None, :], w_dkv, g_kv[None, :], tab)


def attn_body(core_ref, lo_ref, mid_ref, blk_ref, kvr_ref, cqa_ref, cqb_ref, taba_ref, tabb_ref, start_ref,
              wuq_ref, wukv_ref, o_ref, kcat, vt, qcat, sbuf, mbuf, acc, cos_ref, sin_ref, *, kb):
    i = pl.program_id(0)
    tok = kvr_ref.shape[0]
    qb = cqa_ref.shape[0]
    cur, prev = i % 2, (i + 1) % 2
    v_new, v_old = i % 3, (i + 1) % 3
    n_piece = tok // kb

    @pl.when(i == 0)
    def _():
        for par in range(2):
            for h in range(2):
                kcat[par, h, :, NOPE_DIM:] = kvr_ref[:, KV_LATENT:]
        for b, tab in enumerate((taba_ref, tabb_ref)):
            rows = pl.ds(b * qb, qb)
            cosine, sine = tab[:, :ROPE_DIM // 2], tab[:, ROPE_DIM // 2:ROPE_DIM]
            cos_ref[rows, :] = jnp.concatenate([cosine] * 4, axis=1)
            sin_ref[rows, :] = jnp.concatenate([-sine, sine, -sine, sine], axis=1)

    def kv_piece(pc):
        rows = pl.ds(pl.multiple_of(pc * kb, kb), kb)
        e = jnp.dot(kvr_ref[rows, :KV_LATENT], wukv_ref[...], preferred_element_type=F32).astype(BF16)
        for h in range(2):
            kcat[cur, h, rows, :NOPE_DIM] = e[:, KV_DIM * h:KV_DIM * h + NOPE_DIM]
            vt[v_new, h, :, rows] = e[:, KV_DIM * h + NOPE_DIM:KV_DIM * (h + 1)].T

    def q_piece():
        for b, cq in enumerate((cqa_ref, cqb_ref)):
            rows = pl.ds(b * qb, qb)
            q = jnp.dot(cq[...], wuq_ref[...], preferred_element_type=F32)
            q_r = jnp.concatenate([q[:, NOPE_DIM:QK_DIM], q[:, QK_DIM + NOPE_DIM:]], axis=1)
            lane = lax.broadcasted_iota(jnp.int32, q_r.shape, 1)
            lo_half = (lane % ROPE_DIM) < (ROPE_DIM // 2)
            swapped = jnp.where(lo_half, pltpu.roll(q_r, 2 * ROPE_DIM - ROPE_DIM // 2, 1),
                                pltpu.roll(q_r, ROPE_DIM // 2, 1))
            q_r = (q_r * cos_ref[rows, :] + swapped * sin_ref[rows, :]).astype(BF16)
            zero = jnp.zeros((qb, ROPE_DIM), BF16)
            for h in range(2):
                qcat[cur, b, h, :, :NOPE_DIM] = q[:, QK_DIM * h:QK_DIM * h + NOPE_DIM].astype(BF16)
                qcat[cur, b, h, :, NOPE_DIM:] = jnp.concatenate([q_r[:, ROPE_DIM * h:ROPE_DIM * (h + 1)], zero], axis=1)

    @pl.when(i == 0)
    def _():
        q_piece()
        lax.fori_loop(0, n_piece, lambda pc, c: (kv_piece(pc), c)[1], 0)

    @pl.when(i > 0)
    def _():
        base = 0
        for b in range(2):
            t0 = blk_ref[b] * qb
            lo = lo_ref[b]
            last = (t0 + qb - 1) // kb

            def step(j, carry, masked, piece, b=b, t0=t0):
                k0 = pl.multiple_of(j * kb, kb)
                krows = pl.ds(k0, kb)
                new = []
                for h in range(2):
                    m, l = carry[2 * h], carry[2 * h + 1]
                    p = jnp.exp2(sbuf[b, h, krows, :] - mbuf[b, h])
                    s = lax.dot_general(kcat[prev, h, krows, :], qcat[prev, b, h], (((1,), (1,)), ((), ())),
                                        preferred_element_type=F32)
                    s = s * (SCORE_SCALE * LOG2E)
                    if masked:
                        r = k0 + lax.broadcasted_iota(jnp.int32, s.shape, 0)
                        t = t0 + lax.broadcasted_iota(jnp.int32, s.shape, 1)
                        s = jnp.where((r <= t) & (r >= start_ref[b]), s, NEG)
                    m = jnp.maximum(m, jnp.max(s.reshape(kb // 8, 8, qb), axis=0))
                    l = l + jnp.sum(p.reshape(kb // 8, 8, qb), axis=0)
                    acc[h] += jnp.dot(vt[v_old, h, :, krows], p.astype(BF16), preferred_element_type=F32)
                    sbuf[b, h, krows, :] = s
                    new += [m, l]
                piece(j)
                return tuple(new)

            piece = lambda j, off=base - lo: kv_piece(off + j)
            acc[...] = jnp.zeros_like(acc)
            carry = (jnp.full((8, qb), NEG, F32), jnp.zeros((8, qb), F32)) * 2
            carry = lax.fori_loop(lo, mid_ref[b], functools.partial(step, masked=True, piece=piece), carry)
            carry = lax.fori_loop(mid_ref[b], last, functools.partial(step, masked=False, piece=piece), carry)
            carry = step(last, carry, True, piece if b == 0 else lambda j: q_piece())
            base = base + (last - lo + 1 if b == 0 else last - lo)
            for h in range(2):
                mbuf[b, h] = jnp.max(carry[2 * h], axis=0, keepdims=True)
                l = jnp.sum(carry[2 * h + 1], axis=0, keepdims=True)
                o = (acc[h] * (1.0 / l)).astype(BF16)
                o_ref[pl.ds(b * qb, qb), VALUE_DIM * h:VALUE_DIM * (h + 1)] = o.T
        lax.fori_loop(base, n_piece, lambda pc, c: (kv_piece(pc), c)[1], 0)


def attention(core, lo, mid, blk, kvr, cqa, cqb, taba, tabb, start, w_uq, w_ukv, kb):
    tok = kvr.shape[0]
    qb, q_lat = cqa.shape
    heads = w_uq.shape[1] // QK_DIM
    pairs = heads // 4
    full = lambda shape: pl.BlockSpec(shape, lambda i, *_: (0,) * len(shape), pipeline_mode=pl.Buffered(1))
    group = lambda i, core: core[0] * pairs + jnp.minimum(i, pairs - 1)
    return pl.pallas_call(
        functools.partial(attn_body, kb=kb),
        grid_spec=pltpu.PrefetchScalarGridSpec(
            num_scalar_prefetch=4,
            grid=(pairs + 2,),
            in_specs=[
                full(kvr.shape), full(cqa.shape), full(cqb.shape), full(taba.shape), full(tabb.shape), full(start.shape),
                pl.BlockSpec((q_lat, 2 * QK_DIM), lambda i, core, *_: (0, group(i, core))),
                pl.BlockSpec((KV_LATENT, 2 * KV_DIM), lambda i, core, *_: (0, group(i, core))),
            ],
            out_specs=pl.BlockSpec((2 * qb, 2 * VALUE_DIM), lambda i, *_: (0, jnp.maximum(i - 2, 0))),
            scratch_shapes=[
                pltpu.VMEM((2, 2, tok, 2 * NOPE_DIM), BF16),
                pltpu.VMEM((3, 2, VALUE_DIM, tok), BF16),
                pltpu.VMEM((2, 2, 2, qb, 2 * NOPE_DIM), BF16),
                pltpu.VMEM((2, 2, tok, qb), F32),
                pltpu.VMEM((2, 2, 1, qb), F32),
                pltpu.VMEM((2, VALUE_DIM, qb), F32),
                pltpu.VMEM((2 * qb, 2 * ROPE_DIM), F32),
                pltpu.VMEM((2 * qb, 2 * ROPE_DIM), F32),
            ]),
        out_shape=jax.ShapeDtypeStruct((2 * qb, heads // 2 * VALUE_DIM), BF16),
        compiler_params=pltpu.CompilerParams(dimension_semantics=("arbitrary",), vmem_limit_bytes=62 * 2 ** 20),
        cost_estimate=pl.CostEstimate(flops=80 * 10 ** 9, bytes_accessed=45 * 10 ** 6, transcendentals=40 * 10 ** 6),
    )(core, lo, mid, blk, kvr, cqa, cqb, taba, tabb, start, w_uq, w_ukv)


def tail_body(chips, o_hbm, wo_hbm, wg_hbm, wg2_hbm, wu_hbm, wu2_hbm, wd_hbm, wd2_hbm, g_ref, out_ref,
              obuf, wbuf, acc, xr, yall, hbuf, wg, wu, act, rsr, rss,
              o_sem, w_sem, f_sem, d_sem, xs_sem, xr_sem, as_sem, ar_sem, fs_sem, fr_sem, ss_sem, sr_sem):
    me = lax.axis_index('sp')
    chip, core = me // 2, me % 2
    right, left = (chip + 1) % chips, (chip + chips - 1) % chips
    far = (chip + 2) % chips
    ring = (2 * right + core, 2 * left + core)
    peer = 2 * chip + 1 - core
    src = (left, right)
    nt, kt = acc.shape[0], obuf.shape[1] // wbuf.shape[1]
    nbuf, tk, tn = wbuf.shape
    blk = yall.shape[2]
    half = blk // 2
    depth = kt * tk
    shard = wg_hbm.shape[1]

    def slot_of(q):
        return core * (chips - 1) + (1 - 2 * core) * q

    def remote(s, d, ssem, rsem, dev):
        return pltpu.make_async_remote_copy(src_ref=s, dst_ref=d, send_sem=ssem, recv_sem=rsem,
                                            device_id={'sp': dev}, device_id_type=pl.DeviceIdType.MESH)

    def w_copy(t):
        n, k = t // kt, t % kt
        return pltpu.make_async_copy(
            wo_hbm.at[pl.ds(pl.multiple_of(core * depth + k * tk, tk), tk), pl.ds(pl.multiple_of(n * tn, tn), tn)],
            wbuf.at[t % nbuf], w_sem.at[t % nbuf])

    def o_copy(k):
        cols = pl.ds(pl.multiple_of(k * tk, tk), tk)
        return pltpu.make_async_copy(o_hbm.at[:, cols], obuf.at[:, cols], o_sem.at[k])

    f_copies = [pltpu.make_async_copy(s, d.at[:, pl.ds(c * shard, shard)], f_sem.at[i])
                for i, (s, d, c) in enumerate(((wg_hbm, wg, 0), (wg2_hbm, wg, 1), (wu_hbm, wu, 0), (wu2_hbm, wu, 1)))]
    grain = 256
    width = nt * tn
    n_grain = 2 * shard // grain
    per = obuf.shape[0] // grain
    d_copies = []
    for g in range(n_grain):
        s = wd_hbm if g < n_grain // 2 else wd2_hbm
        d_copies.append(pltpu.make_async_copy(
            s.at[pl.ds((g % (n_grain // 2)) * grain, grain), :],
            obuf.at[pl.ds((g % per) * grain, grain), pl.ds((g // per) * width, width)], d_sem.at[g]))

    for k in range(kt):
        o_copy(k).start()
    for t in range(nbuf - 1):
        w_copy(t).start()

    barrier = pltpu.get_barrier_semaphore()
    for dev in (peer,) + ring:
        pl.semaphore_signal(barrier, inc=1, device_id={'sp': dev}, device_id_type=pl.DeviceIdType.MESH)
    pl.semaphore_wait(barrier, 3)

    own_rows = pl.ds(pl.multiple_of(core * blk, blk), blk)
    peer_rows = pl.ds(pl.multiple_of((1 - core) * blk, blk), blk)

    def x_copy(n):
        return remote(acc.at[n, peer_rows, :], xr.at[n], xs_sem.at[n], xr_sem.at[n], peer)

    def a_copy(d, n, slot):
        return remote(yall.at[slot, n], yall.at[slot, n], as_sem.at[d, n], ar_sem.at[d, n], ring[d])

    def f_copy(d, n, slot):
        rows = pl.ds(d * half, half)
        return remote(yall.at[slot, n, rows, :], yall.at[slot, n, rows, :], fs_sem.at[d, n], fr_sem.at[d, n], ring[d])

    def combine(n):
        x_copy(n).wait_recv()
        yall[chip, n] = (acc[n, own_rows, :] + xr[n]).astype(BF16)
        for d in range(2):
            a_copy(d, n, chip).start()

    def forward(n):
        for d in range(2):
            a_copy(d, n, src[d]).wait_recv()
            f_copy(d, n, src[d]).start()

    def w_step(t, _):
        n, k = t // kt, t % kt

        @pl.when(t + nbuf - 1 < nt * kt)
        def _():
            w_copy(t + nbuf - 1).start()

        @pl.when(t == nbuf)
        def _():
            for c in f_copies:
                c.start()

        @pl.when(n == 0)
        def _():
            o_copy(k).wait()
        w_copy(t).wait()
        prod = jnp.dot(obuf[:, pl.ds(pl.multiple_of(k * tk, tk), tk)], wbuf[t % nbuf], preferred_element_type=F32)

        @pl.when(k == 0)
        def _():
            acc[n] = prod

        @pl.when(k > 0)
        def _():
            acc[n] += prod

        @pl.when((k == kt // 2) & (n >= 1))
        def _():
            combine(n - 1)

        @pl.when(k == kt - 1)
        def _():
            x_copy(n).start()

            @pl.when(n >= 3)
            def _():
                forward(n - 3)
        return 0

    lax.fori_loop(0, nt * kt, w_step, 0)
    for c in d_copies:
        c.start()
    combine(nt - 1)
    forward(nt - 3)

    def activate(slot):
        def norm(r, _):
            rows = pl.ds(pl.multiple_of(r * 64, 64), 64)
            ys = [yall[slot, k, rows, :].astype(F32) for k in range(nt)]
            total = sum(jnp.sum(y * y, axis=-1, keepdims=True) for y in ys)
            scale = lax.rsqrt(total * (1.0 / width) + 1e-6)
            for k in range(nt):
                gain = g_ref[:, pl.ds(k * tn, tn)].astype(F32)
                hbuf[k, rows, :] = (ys[k] * scale * gain).astype(BF16)
            return 0
        lax.fori_loop(0, blk // 64, norm, 0)

        def cols(c, _):
            cs = pl.ds(pl.multiple_of(c * 256, 256), 256)
            gate = sum(jnp.dot(hbuf[k], wg[pl.ds(k * tn, tn), cs], preferred_element_type=F32) for k in range(nt))
            up = sum(jnp.dot(hbuf[k], wu[pl.ds(k * tn, tn), cs], preferred_element_type=F32) for k in range(nt))
            act[slot, :, cs] = (jax.nn.silu(gate) * up).astype(BF16)
            return 0
        lax.fori_loop(0, 2 * shard // 256, cols, 0)

    hw = width // 2

    def down(slot, c, d):
        rows = pl.ds(c * half, half)
        return sum(jnp.dot(act[slot, rows, pl.ds(g * grain, grain)],
                           obuf[pl.ds((g % per) * grain, grain),
                                pl.ds(pl.multiple_of((g // per) * width + d * hw, 256), hw)],
                           preferred_element_type=F32) for g in range(n_grain))

    def s_copy(d, s, c):
        src_ref = rss.at[d, c] if s == 0 else rsr.at[d, s - 1, c]
        return remote(src_ref, rsr.at[d, s, c], ss_sem.at[d, s, c], sr_sem.at[d, s, c], ring[0] + d * (ring[1] - ring[0]))

    def first(d):
        for c in range(2):
            rss[d, c] = down(slot_of(left + d * (right - left)), c, d)
            s_copy(d, 0, c).start()

    for c in f_copies:
        c.wait()
    activate(chip)
    forward(nt - 2)
    forward(nt - 1)
    for c in d_copies:
        c.wait()
    activate(left)

    @pl.when(core == 0)
    def _():
        first(0)
    activate(right)
    parity = chip % 2
    first(core * parity + (1 - core))
    for n in range(nt):
        for d in range(2):
            f_copy(d, n, far).wait_recv()
    activate(far)

    @pl.when(core == 1)
    def _():
        first(1 - parity)

    for s, dests in ((1, (far, far)), (2, (right, left))):
        for c in range(2):
            for d in range(2):
                part = down(slot_of(dests[d]), c, d)
                s_copy(d, s - 1, c).wait_recv()
                rsr[d, s - 1, c] = rsr[d, s - 1, c] + part
                s_copy(d, s, c).start()

    mine = slot_of(chip)
    per_half = hw // half
    for c in range(2):
        rows = pl.ds(c * half, half)
        for d in range(2):
            part = down(mine, c, d)
            s_copy(d, 2, c).wait_recv()
            pieces = []
            for col in range(d * hw, (d + 1) * hw, 256):
                pieces.append(yall[mine, col // tn, rows, pl.ds(col % tn, 256)].astype(F32))
            y = jnp.concatenate(pieces, axis=1)
            out_ref[rows, pl.ds(d * hw, hw)] = (y + (rsr[d, 2, c] + part)).astype(BF16)

    for n in range(nt):
        x_copy(n).wait_send()
        for d in range(2):
            a_copy(d, n, chip).wait_send()
            f_copy(d, n, src[d]).wait_send()
    for d in range(2):
        for s in range(3):
            for c in range(2):
                s_copy(d, s, c).wait_send()


def tail(chips, o, w_o, w_gate, w_gate2, w_up, w_up2, w_down, w_down2, g_ffn, nbuf=4, tk=1024, tn=512):
    rows, depth = o.shape
    width = w_o.shape[1]
    shard = w_gate.shape[1]
    blk = rows // 2
    nt, kt = width // tn, depth // tk
    dma = pltpu.SemaphoreType.DMA
    hbm = pl.BlockSpec(memory_space=pl.ANY)
    vmem = pl.BlockSpec(memory_space=pltpu.VMEM)
    return pl.pallas_call(
        functools.partial(tail_body, chips),
        in_specs=[hbm] * 8 + [vmem],
        out_specs=vmem,
        out_shape=jax.ShapeDtypeStruct((blk, width), BF16),
        scratch_shapes=[
            pltpu.VMEM((rows, depth), BF16),
            pltpu.VMEM((nbuf, tk, tn), BF16),
            pltpu.VMEM((nt, rows, tn), F32),
            pltpu.VMEM((nt, blk, tn), F32),
            pltpu.VMEM((chips, nt, blk, tn), BF16),
            pltpu.VMEM((nt, blk, tn), BF16),
            pltpu.VMEM((width, 2 * shard), BF16),
            pltpu.VMEM((width, 2 * shard), BF16),
            pltpu.VMEM((chips, blk, 2 * shard), BF16),
            pltpu.VMEM((2, 3, 2, blk // 2, width // 2), F32),
            pltpu.VMEM((2, 2, blk // 2, width // 2), F32),
            dma((kt,)), dma((nbuf,)), dma((4,)), dma((2 * shard // 256,)),
            dma((nt,)), dma((nt,)), dma((2, nt)), dma((2, nt)), dma((2, nt)), dma((2, nt)),
            dma((2, 3, 2)), dma((2, 3, 2)),
        ],
        compiler_params=pltpu.CompilerParams(collective_id=0, has_side_effects=True,
                                             vmem_limit_bytes=63 * 2 ** 20),
        cost_estimate=pl.CostEstimate(flops=46 * 10 ** 9, bytes_accessed=75 * 10 ** 6, transcendentals=10 ** 6),
    )(o, w_o, w_gate, w_gate2, w_up, w_up2, w_down, w_down2, g_ffn)


def solution(mesh):
    group_size = mesh.shape['sp']
    chips = group_size // 2
    tok_spec = P(('dp', 'sp'), None)
    row_spec = P(('dp', 'sp'))
    full_spec = P()
    col_spec = P(None, 'sp')
    swap = [(d, d ^ 1) for d in range(group_size)]

    def device_fn(x_blk, seg_blk, pos_blk, w_dq, g_q, w_uq, w_dkv, g_kv, w_ukv, w_o, g_ffn, w_gate, w_up, w_down):
        me = lax.axis_index('sp')
        chip, core = me // 2, me % 2
        blk_len = x_blk.shape[0]
        core_arr = core.reshape(1).astype(jnp.int32)

        cosine, sine = rope_tables(pos_blk)
        tab = jnp.concatenate([cosine, sine, jnp.broadcast_to(pos_blk.astype(F32)[:, None], (blk_len, ROPE_DIM))], axis=1)
        kvr, cqa, cqb, taba, tabb = latents(chips, x_blk, w_dq, g_q, w_dkv.T, g_kv, tab)
        kvr, late_gate, late_up, late_down = lax.optimization_barrier((kvr, w_gate, w_up, w_down))
        w_gate2 = lax.ppermute(late_gate, 'sp', swap)
        w_up2 = lax.ppermute(late_up, 'sp', swap)
        w_down2 = lax.ppermute(late_down, 'sp', swap)

        blk = jnp.stack([2 * chip, group_size - 1 - 2 * chip]).astype(jnp.int32)
        pos_q = jnp.stack([taba[:, ROPE_DIM], tabb[:, ROPE_DIM]]).astype(jnp.int32)
        start = blk[:, None] * blk_len + jnp.arange(blk_len, dtype=jnp.int32)[None, :] - pos_q
        kb = 2 * blk_len
        start = start.reshape(2, 1, blk_len)
        lo = start[:, 0, 0] // kb
        last = (blk * blk_len + blk_len - 1) // kb
        mid = jnp.maximum(jnp.minimum((start[:, 0, -1] + kb - 1) // kb, last), lo)

        o = attention(core_arr, lo, mid, blk, kvr, cqa, cqb, taba, tabb, start, w_uq, w_ukv, kb)
        return tail(chips, o, w_o, w_gate, w_gate2, w_up, w_up2, w_down, w_down2, g_ffn[None, :])

    return jax.shard_map(device_fn, mesh=mesh, in_specs=(tok_spec, row_spec, row_spec, full_spec, full_spec, full_spec, full_spec, full_spec, full_spec, full_spec, full_spec, col_spec, col_spec, P('sp', None)), out_specs=tok_spec, check_vma=False)
```
